32 devices in a mesh: fields: 1 (over z), col: 4 (over y), row: 8 (over x, core).
Axes of the slice: x: 4, y: 4, z: 1, core: 2. Of those that a mesh axis runs over, the one named last changes fastest.
The devices are a block of a 4x4x8 slice.
Arguments:
- field_u: bfloat16 [1, 512, 512, 512], P('fields', None, 'row', 'col')
- fac_a: bfloat16 [512, 512], P('fields')
- fac_b: bfloat16 [512, 512], P('fields')
- fac_c: bfloat16 [512, 512], P('fields')
- diag_d: float32 [512, 512, 512], P(('fields', 'row'), 'col')
Outputs:
- output: float32 [1, 512, 512, 512], P('fields', None, 'row', 'col')
All inputs are finite; a program needn't handle non-finite values.
Results may differ from the reference program's by a relative error of at most 0.00303378.
Values are sent between devices in bfloat16 or wider.
A program may use at most 768 MiB of HBM per device.

```python
import jax
import jax.numpy as jnp
from jax import lax

N = 512
BATCH = 1


def setup_inputs(seed: int = 0, part: int = 0) -> dict:
    base_key = jax.random.fold_in(jax.random.key(seed), part)
    key_field, key_a, key_b, key_c, key_diag = jax.random.split(base_key, 5)
    fan_scale = N ** -0.5
    field_u = jax.random.normal(key_field, (BATCH, N, N, N), jnp.float32)
    fac_a = jax.random.normal(key_a, (N, N), jnp.float32) * fan_scale
    fac_b = jax.random.normal(key_b, (N, N), jnp.float32) * fan_scale
    fac_c = jax.random.normal(key_c, (N, N), jnp.float32) * fan_scale
    diag_d = jnp.exp(0.5 * jax.random.normal(key_diag, (N, N, N), jnp.float32))
    return {"field_u": field_u.astype(jnp.bfloat16), "fac_a": fac_a.astype(jnp.bfloat16), "fac_b": fac_b.astype(jnp.bfloat16), "fac_c": fac_c.astype(jnp.bfloat16), "diag_d": diag_d}


def reference(field_u, fac_a, fac_b, fac_c, diag_d):
    mat_a = fac_a.astype(jnp.float32)
    mat_b = fac_b.astype(jnp.float32)
    mat_c = fac_c.astype(jnp.float32)
    scales = diag_d.astype(jnp.float32)

    def to_bf16(values_in):
        return values_in.astype(jnp.bfloat16).astype(jnp.float32)

    def one_tensor(tensor):
        stage_one = to_bf16(jnp.einsum("ix,xyz->iyz", mat_a, tensor.astype(jnp.float32)))
        stage_two = to_bf16(jnp.einsum("jy,iyz->ijz", mat_b, stage_one))
        stage_three = to_bf16(jnp.einsum("kz,ijz->ijk", mat_c, stage_two) * scales)
        stage_four = to_bf16(jnp.einsum("kz,ijk->ijz", mat_c, stage_three))
        stage_five = to_bf16(jnp.einsum("jy,ijz->iyz", mat_b, stage_four))
        return jnp.einsum("ix,iyz->xyz", mat_a, stage_five)

    return lax.map(one_tensor, field_u)
```

```python
import functools

import jax
import jax.numpy as jnp
from jax import lax
from jax.experimental import pallas as pl
from jax.experimental.pallas import tpu as pltpu
from jax.sharding import PartitionSpec as P

MESH = pl.DeviceIdType.MESH
F32, BF16 = jnp.float32, jnp.bfloat16
CI = 8
TY = 16


def dot(a, b):
    return jnp.dot(a, b, preferred_element_type=F32)


def exchange_kernel(R, C, u, a, b, bt, c, ct, d, h5, ubuf, sa, sb, tx1, rx1, tx2, rx2, tx3, rx3, tx4, dbuf,
                    usem, dsem, s1, r1, s2, r2, s3, r3, s4, r4, lsem):
    X, Y, Z = u.shape
    J, I = d.shape[1], d.shape[0]
    N = X
    n = I // CI
    me_r, me_c = lax.axis_index("row"), lax.axis_index("col")

    def row_peer(off):
        return lax.rem(me_r + off, R)

    def col_peer(off):
        return lax.rem(me_c + off, C)

    def load_u(t):
        return pltpu.make_async_copy(u.at[:, pl.ds(t * TY, TY), :], ubuf.at[t % 2], usem.at[t % 2])

    def load_d(k, slot):
        return pltpu.make_async_copy(d.at[pl.ds(k * CI, CI)], dbuf.at[slot], dsem.at[slot])

    load_u(0).start()
    load_u(1).start()
    load_d(0, 0).start()

    barrier = pltpu.get_barrier_semaphore()
    for off in range(1, R):
        pl.semaphore_signal(barrier, inc=1, device_id={"row": row_peer(off)}, device_id_type=MESH)
    for off in range(1, C):
        pl.semaphore_signal(barrier, inc=1, device_id={"col": col_peer(off)}, device_id_type=MESH)

    def send_row(k, y0, ny):
        for off in range(1, R):
            p = row_peer(off)
            pltpu.make_async_remote_copy(
                src_ref=tx1.at[pl.ds(p * I + k * CI, CI), pl.ds(y0, ny), :],
                dst_ref=rx1.at[k, :, pl.ds(pl.multiple_of(me_r * Y + y0, TY), ny), :],
                send_sem=s1, recv_sem=r1.at[k], device_id={"row": p}, device_id_type=MESH).start()

    def keep_row(k):
        y0 = pl.multiple_of(me_r * Y, Y)
        rx1[k, :, pl.ds(y0, Y), :] = tx1[pl.ds(me_r * I + k * CI, CI), :, :]

    for t in range(Y // TY):
        load_u(t).wait()
        slot = t % 2

        def spread(g, _):
            x0 = g * 32
            v = ubuf[slot, pl.ds(x0, 32)].astype(F32)
            for h in range(TY // 8):
                sa[h, pl.ds(pl.multiple_of(x0 * 8, 256), 256), :] = v[:, h * 8:(h + 1) * 8, :].reshape(256, Z)
            return 0

        lax.fori_loop(0, X // 32, spread, 0)
        if t + 2 < Y // TY:
            load_u(t + 2).start()
        for h in range(TY // 8):
            def pair(q, _):
                y = 2 * q
                rhs = jnp.concatenate(
                    [sa[h, pl.ds(y, X, stride=8), :].astype(BF16), sa[h, pl.ds(y + 1, X, stride=8), :].astype(BF16)], axis=1)
                res = dot(a[...], rhs)
                sb[h, pl.ds(y, N, stride=8), :] = res[:, :Z]
                sb[h, pl.ds(y + 1, N, stride=8), :] = res[:, Z:]
                return 0

            lax.fori_loop(0, 4, pair, 0)

        def gather(g, _):
            i0 = g * 32
            parts = [sb[h, pl.ds(pl.multiple_of(i0 * 8, 256), 256), :].reshape(32, 8, Z) for h in range(TY // 8)]
            tx1[pl.ds(i0, 32), pl.ds(t * TY, TY), :] = jnp.concatenate(parts, axis=1).astype(BF16)
            return 0

        lax.fori_loop(0, N // 32, gather, 0)
        if t == 0:
            pl.semaphore_wait(barrier, R - 1 + C - 1)
        send_row(0, t * TY, TY)

    def rest(k, _):
        send_row(k, 0, Y)
        return 0

    lax.fori_loop(1, n, rest, 0)

    def own(k, _):
        keep_row(k)
        return 0

    lax.fori_loop(0, n, own, 0)

    def wait_bytes(ref, sem):
        pltpu.make_async_copy(ref, ref, sem).wait()

    def step(k, _):
        @pl.when(k < n)
        def _():
            wait_bytes(rx1.at[k, pl.ds(0, CI * (R - 1) // R)], r1.at[k])
            slot = lax.rem(k, 2)

            @pl.when(k >= 2)
            def _():
                wait_bytes(tx2.at[slot, :, pl.ds(0, J * (C - 1)), :], s2.at[slot])

            def pair(q, _):
                i = 2 * q
                rhs = jnp.concatenate([rx1[k, i], rx1[k, i + 1]], axis=1)
                res = dot(b[...], rhs).astype(BF16)
                tx2[slot, i] = res[:, :Z]
                tx2[slot, i + 1] = res[:, Z:]
                return 0

            lax.fori_loop(0, CI // 2, pair, 0)
            for off in range(1, C):
                p = col_peer(off)
                pltpu.make_async_remote_copy(
                    src_ref=tx2.at[slot, :, pl.ds(pl.multiple_of(p * J, J), J), :], dst_ref=rx2.at[k, me_c],
                    send_sem=s2.at[slot], recv_sem=r2.at[k], device_id={"col": p}, device_id_type=MESH).start()
            rx2[k, me_c] = tx2[slot, :, pl.ds(pl.multiple_of(me_c * J, J), J), :]

        @pl.when(jnp.logical_and(k >= 1, k < n + 1))
        def _():
            m = k - 1
            slot = lax.rem(m, 2)

            @pl.when(m + 1 < n)
            def _():
                load_d(m + 1, 1 - slot).start()

            load_d(m, slot).wait()
            wait_bytes(rx2.at[m, pl.ds(0, C - 1)], r2.at[m])

            @pl.when(m >= 2)
            def _():
                wait_bytes(tx3.at[slot, pl.ds(0, C - 1)], s3.at[slot])

            def pair(q, _):
                i = 2 * q
                lhs = jnp.concatenate([rx2[m, e, pl.ds(i, 2)].reshape(2 * J, Z) for e in range(C)], axis=1)
                h3 = (dot(lhs, ct[...]) * dbuf[slot, pl.ds(i, 2)].reshape(2 * J, N)).astype(BF16)
                h4 = dot(h3, c[...]).astype(BF16)
                for e in range(C):
                    tx3[slot, e, pl.ds(i, 2)] = h4[:, e * Z:(e + 1) * Z].reshape(2, J, Z)
                return 0

            lax.fori_loop(0, CI // 2, pair, 0)
            for off in range(1, C):
                p = col_peer(off)
                pltpu.make_async_remote_copy(
                    src_ref=tx3.at[slot, p], dst_ref=rx3.at[m, :, pl.ds(pl.multiple_of(me_c * J, J), J), :],
                    send_sem=s3.at[slot], recv_sem=r3.at[m], device_id={"col": p}, device_id_type=MESH).start()
            rx3[m, :, pl.ds(pl.multiple_of(me_c * J, J), J), :] = tx3[slot, me_c]

        @pl.when(k >= 2)
        def _():
            m = k - 2
            slot = lax.rem(m, 2)
            wait_bytes(rx3.at[m, :, pl.ds(0, J * (C - 1)), :], r3.at[m])

            def own_copy(m, slot):
                return pltpu.make_async_copy(
                    tx4.at[slot, pl.ds(pl.multiple_of(me_r * Y, Y), Y)],
                    h5.at[:, pl.ds(pl.multiple_of(me_r * I + m * CI, CI), CI), :], lsem.at[slot])

            @pl.when(m >= 2)
            def _():
                wait_bytes(tx4.at[slot, pl.ds(0, Y * (R - 1))], s4.at[slot])
                own_copy(m - 2, slot).wait()

            def pair(q, _):
                i = 2 * q
                rhs = jnp.concatenate([rx3[m, i], rx3[m, i + 1]], axis=1)
                res = dot(bt[...], rhs)
                sa[0, pl.ds(i, N, stride=8), :] = res[:, :Z]
                sa[0, pl.ds(i + 1, N, stride=8), :] = res[:, Z:]
                return 0

            lax.fori_loop(0, CI // 2, pair, 0)

            def pack(g, _):
                y0 = g * 32
                tx4[slot, pl.ds(y0, 32)] = sa[0, pl.ds(pl.multiple_of(y0 * 8, 256), 256), :].reshape(32, 8, Z).astype(BF16)
                return 0

            lax.fori_loop(0, N // 32, pack, 0)
            for off in range(1, R):
                p = row_peer(off)
                pltpu.make_async_remote_copy(
                    src_ref=tx4.at[slot, pl.ds(pl.multiple_of(p * Y, Y), Y)],
                    dst_ref=h5.at[:, pl.ds(pl.multiple_of(me_r * I + m * CI, CI), CI), :],
                    send_sem=s4.at[slot], recv_sem=r4, device_id={"row": p}, device_id_type=MESH).start()
            own_copy(m, slot).start()

        return 0

    lax.fori_loop(0, n + 2, step, 0)

    wait_bytes(tx1.at[pl.ds(0, I * (R - 1))], s1)
    for m in (n - 2, n - 1):
        slot = m % 2
        wait_bytes(tx2.at[slot, :, pl.ds(0, J * (C - 1)), :], s2.at[slot])
        wait_bytes(tx3.at[slot, pl.ds(0, C - 1)], s3.at[slot])
        wait_bytes(tx4.at[slot, pl.ds(0, Y * (R - 1))], s4.at[slot])
        pltpu.make_async_copy(
            tx4.at[slot, pl.ds(0, Y)], h5.at[:, pl.ds(0, CI), :], lsem.at[slot]).wait()
    pltpu.make_async_copy(h5.at[:, pl.ds(0, I * (R - 1)), :], h5.at[:, pl.ds(0, I * (R - 1)), :], r4).wait()


def exchange(R, C, u, a, b, bt, c, ct, d):
    X, Y, Z = u.shape
    I, J, N = d.shape
    n = I // CI
    vm = pl.BlockSpec(memory_space=pltpu.VMEM)
    hb = pl.BlockSpec(memory_space=pl.ANY)
    DMA = pltpu.SemaphoreType.DMA
    return pl.pallas_call(
        functools.partial(exchange_kernel, R, C),
        name="exchange",
        out_shape=jax.ShapeDtypeStruct((Y, N, Z), BF16),
        in_specs=[hb, vm, vm, vm, vm, vm, hb],
        out_specs=hb,
        scratch_shapes=[
            pltpu.VMEM((2, X, TY, Z), BF16),
            pltpu.VMEM((TY // 8, X * 8, Z), F32),
            pltpu.VMEM((TY // 8, N * 8, Z), F32),
            pltpu.VMEM((N, Y, Z), BF16),
            pltpu.VMEM((n, CI, N, Z), BF16),
            pltpu.VMEM((2, CI, N, Z), BF16),
            pltpu.VMEM((n, C, CI, J, Z), BF16),
            pltpu.VMEM((2, C, CI, J, Z), BF16),
            pltpu.VMEM((n, CI, N, Z), BF16),
            pltpu.VMEM((2, N, CI, Z), BF16),
            pltpu.VMEM((2, CI, J, N), F32),
            DMA((2,)), DMA((2,)), DMA, DMA((n,)), DMA((2,)), DMA((n,)), DMA((2,)), DMA((n,)), DMA((2,)), DMA, DMA((2,)),
        ],
        compiler_params=pltpu.CompilerParams(
            collective_id=0, has_side_effects=True, vmem_limit_bytes=67043328),
    )(u, a, b, bt, c, ct, d)


def last_kernel(at, h, w):
    TYO = h.shape[0]
    Z = h.shape[2]
    flat = w.reshape(w.shape[0] * TYO, Z)
    X = w.shape[0]
    for q in range(TYO // 2):
        y = 2 * q
        res = dot(at[...], jnp.concatenate([h[y], h[y + 1]], axis=1))
        flat[pl.ds(y, X, stride=TYO), :] = res[:, :Z]
        flat[pl.ds(y + 1, X, stride=TYO), :] = res[:, Z:]


def last(at, h5):
    Y, N, Z = h5.shape
    X = at.shape[0]
    T = 8
    return pl.pallas_call(
        last_kernel,
        name="last",
        grid=(Y // T,),
        out_shape=jax.ShapeDtypeStruct((X, Y, Z), F32),
        in_specs=[pl.BlockSpec((X, N), lambda t: (0, 0)), pl.BlockSpec((T, N, Z), lambda t: (t, 0, 0))],
        out_specs=pl.BlockSpec((X, T, Z), lambda t: (0, t, 0)),
        compiler_params=pltpu.CompilerParams(vmem_limit_bytes=32 * 2**20),
    )(at, h5)


def solution(mesh):
    R, C = mesh.shape["row"], mesh.shape["col"]

    def local_apply(field_u, fac_a, fac_b, fac_c, diag_d):
        outs = []
        for e in range(field_u.shape[0]):
            h5 = exchange(R, C, field_u[e], fac_a, fac_b, fac_b.T, fac_c, fac_c.T, diag_d)
            outs.append(last(fac_a.T, h5))
        return jnp.stack(outs) if len(outs) > 1 else outs[0][None]

    spec = P("fields", None, "row", "col")
    fac = P("fields", None)
    return jax.shard_map(local_apply, mesh=mesh, in_specs=(spec, fac, fac, fac, P(("fields", "row"), "col", None)),
                         out_specs=spec, check_vma=False)
```

```python
import functools

import jax
import jax.numpy as jnp
from jax import lax
from jax.experimental import pallas as pl
from jax.experimental.pallas import tpu as pltpu
from jax.sharding import PartitionSpec as P

MESH = pl.DeviceIdType.MESH
F32, BF16 = jnp.float32, jnp.bfloat16
CI = 2
TY = 16
AHEAD = 4
EARLY = 2
LAG3, LAG5 = 1, 3
SLOTS = 4


def dot(a, b):
    return jnp.dot(a, b, preferred_element_type=F32)


def wait_bytes(ref, sem):
    pltpu.make_async_copy(ref, ref, sem).wait()


def exchange_kernel(R, C, u, a_hbm, b_hbm, c_hbm, d, h5, at_out, mats, ubuf, sa, sb, tx1, rx1, tx2, rx2, tx3, rx3, tx4,
                    dbuf, msem, usem, dsem, s1, r1, s2, r2, s3, r3, s4, r4, lsem, asem):
    X, Y, Z = u.shape
    I, J, N = d.shape
    n = I // CI
    a, b, c, at, bt, ct = (mats.at[e] for e in range(6))
    me_r, me_c = lax.axis_index("row"), lax.axis_index("col")

    def row_peer(off):
        return lax.rem(me_r + off, R)

    def col_peer(off):
        return lax.rem(me_c + off, C)

    def load_u(t):
        return pltpu.make_async_copy(u.at[:, pl.ds(t * TY, TY), :], ubuf.at[t % 2], usem.at[t % 2])

    def load_d(k):
        slot = lax.rem(k, SLOTS)
        return pltpu.make_async_copy(d.at[pl.ds(k * CI, CI)], dbuf.at[slot], dsem.at[slot])

    load_u(0).start()
    loads = [pltpu.make_async_copy(h, mats.at[e], msem.at[e]) for e, h in enumerate((a_hbm, b_hbm, c_hbm))]
    loads[0].start()
    load_u(1).start()
    for e in (1, 2):
        loads[e].start()

    barrier = pltpu.get_barrier_semaphore()
    for off in range(1, R):
        pl.semaphore_signal(barrier, inc=1, device_id={"row": row_peer(off)}, device_id_type=MESH)
    for off in range(1, C):
        pl.semaphore_signal(barrier, inc=1, device_id={"col": col_peer(off)}, device_id_type=MESH)

    def send_row(k, y0, ny):
        for off in range(1, R):
            p = row_peer(off)
            pltpu.make_async_remote_copy(
                src_ref=tx1.at[pl.ds(p * I + k * CI, CI), pl.ds(y0, ny), :],
                dst_ref=rx1.at[k, :, pl.ds(pl.multiple_of(me_r * Y + y0, TY), ny), :],
                send_sem=s1, recv_sem=r1.at[k], device_id={"row": p}, device_id_type=MESH).start()

    for t in range(Y // TY):
        load_u(t).wait()
        slot = t % 2

        def spread(g, _):
            x0 = g * 32
            v = ubuf[slot, pl.ds(x0, 32)].astype(F32)
            for h in range(TY // 8):
                sa[h, pl.ds(pl.multiple_of(x0 * 8, 256), 256), :] = v[:, h * 8:(h + 1) * 8, :].reshape(256, Z)
            return 0

        lax.fori_loop(0, X // 32, spread, 0)
        if t + 2 < Y // TY:
            load_u(t + 2).start()
        if t == 0:
            loads[0].wait()

        def tile(h, _):
            rhs = jnp.concatenate([sa[h, pl.ds(e, X, stride=8), :].astype(BF16) for e in range(8)], axis=1)
            res = dot(a[...], rhs)
            for e in range(8):
                sb[h, pl.ds(e, N, stride=8), :] = res[:, e * Z:(e + 1) * Z]
            return 0

        lax.fori_loop(0, TY // 8, tile, 0)

        def gather(g, _):
            i0 = g * 32
            parts = [sb[h, pl.ds(pl.multiple_of(i0 * 8, 256), 256), :].reshape(32, 8, Z) for h in range(TY // 8)]
            tx1[pl.ds(i0, 32), pl.ds(t * TY, TY), :] = jnp.concatenate(parts, axis=1).astype(BF16)
            return 0

        lax.fori_loop(0, N // 32, gather, 0)
        if t == 0:
            pl.semaphore_wait(barrier, R - 1 + C - 1)
        for k in range(EARLY):
            send_row(k, t * TY, TY)

    for k in range(EARLY, AHEAD):
        send_row(k, 0, Y)
    for k in range(LAG3 + 2):
        load_d(k).start()

    def own(k, _):
        rx1[k, :, pl.ds(pl.multiple_of(me_r * Y, Y), Y), :] = tx1[pl.ds(me_r * I + k * CI, CI), :, :]
        return 0

    lax.fori_loop(0, n, own, 0)
    loads[1].wait()
    loads[2].wait()
    for e in range(3):
        mats[3 + e] = mats[e].T
    save_at = pltpu.make_async_copy(at, at_out, asem)
    save_at.start()

    def own_copy(m, slot):
        return pltpu.make_async_copy(
            tx4.at[slot, :, pl.ds(pl.multiple_of(me_r * Y, Y), Y), :], h5.at[pl.ds(me_r * I + m * CI, CI)], lsem.at[slot])

    def free2(slot):
        wait_bytes(tx2.at[slot, :, pl.ds(0, J * (C - 1)), :], s2.at[slot])

    def free3(slot):
        wait_bytes(tx3.at[slot, pl.ds(0, C - 1)], s3.at[slot])

    def free4(m, slot):
        wait_bytes(tx4.at[slot, :, pl.ds(0, Y * (R - 1)), :], s4.at[slot])
        own_copy(m, slot).wait()

    def step(k, _):
        @pl.when(k + AHEAD < n)
        def _():
            send_row(k + AHEAD, 0, Y)

        @pl.when(k < n)
        def _():
            slot = lax.rem(k, SLOTS)
            wait_bytes(rx1.at[k, :, pl.ds(0, Y * (R - 1)), :], r1.at[k])

            @pl.when(k >= SLOTS)
            def _():
                free2(slot)

            res = dot(b[...], jnp.concatenate([rx1[k, i] for i in range(CI)], axis=1)).astype(BF16)
            for i in range(CI):
                tx2[slot, i] = res[:, i * Z:(i + 1) * Z]
            for off in (2, 1, 3):
                p = col_peer(off)
                pltpu.make_async_remote_copy(
                    src_ref=tx2.at[slot, :, pl.ds(pl.multiple_of(p * J, J), J), :], dst_ref=rx2.at[k, me_c],
                    send_sem=s2.at[slot], recv_sem=r2.at[k], device_id={"col": p}, device_id_type=MESH).start()
            rx2[k, me_c] = tx2[slot, :, pl.ds(pl.multiple_of(me_c * J, J), J), :]

        m = k - LAG3

        @pl.when(jnp.logical_and(m >= 0, m < n))
        def _():
            slot = lax.rem(m, SLOTS)

            @pl.when(m + LAG3 + 2 < n)
            def _():
                load_d(m + LAG3 + 2).start()

            load_d(m).wait()
            wait_bytes(rx2.at[m, pl.ds(0, C - 1)], r2.at[m])

            @pl.when(m >= SLOTS)
            def _():
                free3(slot)

            lhs = jnp.concatenate([rx2[m, e].reshape(CI * J, Z) for e in range(C)], axis=1)
            h3 = (dot(lhs, ct[...]) * dbuf[slot].reshape(CI * J, N)).astype(BF16)
            h4 = dot(h3, c[...]).astype(BF16)
            for e in range(C):
                tx3[slot, e] = h4[:, e * Z:(e + 1) * Z].reshape(CI, J, Z)
            for off in (2, 1, 3):
                p = col_peer(off)
                pltpu.make_async_remote_copy(
                    src_ref=tx3.at[slot, p], dst_ref=rx3.at[m, :, pl.ds(pl.multiple_of(me_c * J, J), J), :],
                    send_sem=s3.at[slot], recv_sem=r3.at[m], device_id={"col": p}, device_id_type=MESH).start()
            rx3[m, :, pl.ds(pl.multiple_of(me_c * J, J), J), :] = tx3[slot, me_c]

        o = k - LAG5

        @pl.when(o >= 0)
        def _():
            slot = lax.rem(o, SLOTS)
            wait_bytes(rx3.at[o, :, pl.ds(0, J * (C - 1)), :], r3.at[o])

            @pl.when(o >= SLOTS)
            def _():
                free4(o - SLOTS, slot)

            res = dot(bt[...], jnp.concatenate([rx3[o, i] for i in range(CI)], axis=1)).astype(BF16)
            for i in range(CI):
                tx4[slot, i] = res[:, i * Z:(i + 1) * Z]
            for off in (4, 5, 3, 2, 6, 7, 1):
                p = row_peer(off)
                pltpu.make_async_remote_copy(
                    src_ref=tx4.at[slot, :, pl.ds(pl.multiple_of(p * Y, Y), Y), :],
                    dst_ref=h5.at[pl.ds(me_r * I + o * CI, CI)],
                    send_sem=s4.at[slot], recv_sem=r4, device_id={"row": p}, device_id_type=MESH).start()
            own_copy(o, slot).start()

        return 0

    lax.fori_loop(0, n + LAG5, step, 0)

    save_at.wait()
    wait_bytes(tx1.at[pl.ds(0, I * (R - 1))], s1)
    for m in range(n - SLOTS, n):
        free2(m % SLOTS)
        free3(m % SLOTS)
        free4(m, m % SLOTS)
    wait_bytes(h5.at[pl.ds(0, I * (R - 1))], r4)


def exchange(R, C, u, a, b, c, d):
    X, Y, Z = u.shape
    I, J, N = d.shape
    n = I // CI
    hb = pl.BlockSpec(memory_space=pl.ANY)
    DMA = pltpu.SemaphoreType.DMA
    return pl.pallas_call(
        functools.partial(exchange_kernel, R, C),
        name="exchange",
        out_shape=(jax.ShapeDtypeStruct((N, Y, Z), BF16), jax.ShapeDtypeStruct((X, N), BF16)),
        in_specs=[hb] * 5,
        out_specs=(hb, hb),
        scratch_shapes=[
            pltpu.VMEM((6, N, X), BF16),
            pltpu.VMEM((2, X, TY, Z), BF16),
            pltpu.VMEM((TY // 8, X * 8, Z), F32),
            pltpu.VMEM((TY // 8, N * 8, Z), F32),
            pltpu.VMEM((N, Y, Z), BF16),
            pltpu.VMEM((n, CI, N, Z), BF16),
            pltpu.VMEM((SLOTS, CI, N, Z), BF16),
            pltpu.VMEM((n, C, CI, J, Z), BF16),
            pltpu.VMEM((SLOTS, C, CI, J, Z), BF16),
            pltpu.VMEM((n, CI, N, Z), BF16),
            pltpu.VMEM((SLOTS, CI, N, Z), BF16),
            pltpu.VMEM((SLOTS, CI, J, N), F32),
            DMA((3,)), DMA((2,)), DMA((SLOTS,)), DMA, DMA((n,)), DMA((SLOTS,)), DMA((n,)), DMA((SLOTS,)), DMA((n,)),
            DMA((SLOTS,)), DMA, DMA((SLOTS,)), DMA,
        ],
        compiler_params=pltpu.CompilerParams(
            collective_id=0, has_side_effects=True, vmem_limit_bytes=67043328),
    )(u, a, b, c, d)


def last_kernel(at, h, w, sa):
    N, T, Z = h.shape
    X = w.shape[0]

    def spread(g, _):
        i0 = g * 32
        sa[pl.ds(pl.multiple_of(i0 * T, 32 * T), 32 * T), :] = h[pl.ds(i0, 32)].astype(F32).reshape(32 * T, Z)
        return 0

    lax.fori_loop(0, N // 32, spread, 0)
    rhs = jnp.concatenate([sa[pl.ds(e, N, stride=T), :].astype(BF16) for e in range(T)], axis=1)
    res = dot(at[...], rhs)
    flat = w.reshape(X * T, Z)
    for e in range(T):
        flat[pl.ds(e, X, stride=T), :] = res[:, e * Z:(e + 1) * Z]


def last(at, h5):
    N, Y, Z = h5.shape
    X = at.shape[0]
    T = 8
    return pl.pallas_call(
        last_kernel,
        name="last",
        grid=(Y // T,),
        out_shape=jax.ShapeDtypeStruct((X, Y, Z), F32),
        in_specs=[pl.BlockSpec((X, N), lambda t: (0, 0)), pl.BlockSpec((N, T, Z), lambda t: (0, t, 0))],
        out_specs=pl.BlockSpec((X, T, Z), lambda t: (0, t, 0)),
        scratch_shapes=[pltpu.VMEM((N * T, Z), F32)],
        compiler_params=pltpu.CompilerParams(vmem_limit_bytes=62 * 2**20),
    )(at, h5)


def solution(mesh):
    R, C = mesh.shape["row"], mesh.shape["col"]

    def local_apply(field_u, fac_a, fac_b, fac_c, diag_d):
        outs = []
        for e in range(field_u.shape[0]):
            h5, at = exchange(R, C, field_u[e], fac_a, fac_b, fac_c, diag_d)
            outs.append(last(at, h5))
        return jnp.stack(outs) if len(outs) > 1 else outs[0][None]

    spec = P("fields", None, "row", "col")
    fac = P("fields", None)
    return jax.shard_map(local_apply, mesh=mesh, in_specs=(spec, fac, fac, fac, P(("fields", "row"), "col", None)),
                         out_specs=spec, check_vma=False)
```

```python
import functools

import jax
import jax.numpy as jnp
from jax import lax
from jax.experimental import pallas as pl
from jax.experimental.pallas import tpu as pltpu
from jax.sharding import PartitionSpec as P

MESH = pl.DeviceIdType.MESH
F32, BF16 = jnp.float32, jnp.bfloat16
CI = 2
TY = 16
GI = 8
AHEAD = 4
EARLY = 2
LAG3, LAG5 = 1, 3
SLOTS = 4


def dot(a, b):
    return jnp.dot(a, b, preferred_element_type=F32)


def wait_bytes(ref, sem):
    pltpu.make_async_copy(ref, ref, sem).wait()


def exchange_kernel(R, C, u, a_hbm, b_hbm, c_hbm, d, h5, h5b, at_out, mats, ubuf, u2, sa, sb, tx1, rx1, tx2, rx2, tx3, rx3,
                    tx4, tx4b, dbuf, msem, usem, dsem, s1, r1, s2, r2, s3, r3, s4, r4, lsem, s5, r5, lsem5, asem):
    X, Y, Z = u.shape
    I, J, N = d.shape
    n = I // CI
    a, b, c, at, bt, ct = (mats.at[e] for e in range(6))
    me_r, me_c = lax.axis_index("row"), lax.axis_index("col")

    def row_peer(off):
        return lax.rem(me_r + off, R)

    def col_peer(off):
        return lax.rem(me_c + off, C)

    def load_u(t):
        return pltpu.make_async_copy(u.at[:, pl.ds(t * TY, TY), :], ubuf.at[t % 2], usem.at[t % 2])

    def load_d(k):
        slot = lax.rem(k, SLOTS)
        return pltpu.make_async_copy(d.at[pl.ds(k * CI, CI)], dbuf.at[slot], dsem.at[slot])

    load_u(0).start()
    loads = [pltpu.make_async_copy(h, mats.at[e], msem.at[e]) for e, h in enumerate((a_hbm, b_hbm, c_hbm))]
    loads[0].start()
    load_u(1).start()
    for e in (1, 2):
        loads[e].start()

    barrier = pltpu.get_barrier_semaphore()
    for off in range(1, R):
        pl.semaphore_signal(barrier, inc=1, device_id={"row": row_peer(off)}, device_id_type=MESH)
    for off in range(1, C):
        pl.semaphore_signal(barrier, inc=1, device_id={"col": col_peer(off)}, device_id_type=MESH)

    def send_row(k, y0, ny):
        for off in range(1, R):
            p = row_peer(off)
            pltpu.make_async_remote_copy(
                src_ref=tx1.at[pl.ds(p * I + k * CI, CI), pl.ds(y0, ny), :],
                dst_ref=rx1.at[k, :, pl.ds(pl.multiple_of(me_r * Y + y0, TY), ny), :],
                send_sem=s1, recv_sem=r1.at[k], device_id={"row": p}, device_id_type=MESH).start()

    H = I // 2

    def project(half, h, rhs):
        res = dot(jnp.concatenate([a[pl.ds(e * I + half * H, H), :] for e in range(R)], axis=0), rhs)
        for e in range(8):
            sb[h, pl.ds(e, R * H, stride=8), :] = res[:, e * Z:(e + 1) * Z]

    def gather(half, t):
        def body(e, _):
            parts = [sb[h, pl.ds(pl.multiple_of(e * H * 8, H * 8), H * 8), :].reshape(H, 8, Z) for h in range(TY // 8)]
            tx1[pl.ds(e * I + half * H, H), pl.ds(pl.multiple_of(t * TY, TY), TY), :] = (
                jnp.concatenate(parts, axis=1).astype(BF16))
            return 0

        lax.fori_loop(0, R, body, 0)

    def second(t):
        def body(h, _):
            project(1, h, u2[t * (TY // 8) + h])
            return 0

        lax.fori_loop(0, TY // 8, body, 0)
        gather(1, t)

    for t in range(Y // TY):
        load_u(t).wait()
        slot = t % 2

        def spread(g, _):
            x0 = g * 32
            v = ubuf[slot, pl.ds(x0, 32)].astype(F32)
            for h in range(TY // 8):
                sa[h, pl.ds(pl.multiple_of(x0 * 8, 256), 256), :] = v[:, h * 8:(h + 1) * 8, :].reshape(256, Z)
            return 0

        lax.fori_loop(0, X // 32, spread, 0)
        if t + 2 < Y // TY:
            load_u(t + 2).start()
        if t == 0:
            loads[0].wait()

        def tile(h, _):
            rhs = jnp.concatenate([sa[h, pl.ds(e, X, stride=8), :].astype(BF16) for e in range(8)], axis=1)
            u2[t * (TY // 8) + h] = rhs
            project(0, h, rhs)
            return 0

        lax.fori_loop(0, TY // 8, tile, 0)
        gather(0, t)
        if t == 0:
            pl.semaphore_wait(barrier, R - 1 + C - 1)
        for k in range(EARLY):
            send_row(k, t * TY, TY)

    for k in range(EARLY, AHEAD):
        send_row(k, 0, Y)
    for k in range(LAG3 + 2):
        load_d(k).start()

    second(0)
    loads[1].wait()
    loads[2].wait()
    af = a[...].astype(F32)
    keep = I - GI
    order = [af[e * I:e * I + keep] for e in range(R)] + [af[e * I + keep:(e + 1) * I] for e in range(R)]
    mats[3] = jnp.concatenate(order, axis=0).T.astype(BF16)
    for e in (1, 2):
        mats[3 + e] = mats[e].T
    save_at = pltpu.make_async_copy(at, at_out, asem)
    save_at.start()

    my_y = pl.ds(pl.multiple_of(me_r * Y, Y), Y)

    def to_h5(g):
        return h5.at[:, pl.ds(pl.multiple_of(me_r * keep + g * GI, GI), GI), :]

    def own_copy(g, slot):
        return pltpu.make_async_copy(tx4.at[slot, my_y], to_h5(g), lsem.at[slot])

    def own_copy_b(q):
        return pltpu.make_async_copy(
            tx4b.at[q, :, my_y, :], h5b.at[pl.ds(me_r * GI + q * CI, CI)], lsem5.at[q])

    def free2(slot):
        wait_bytes(tx2.at[slot, :, pl.ds(0, J * (C - 1)), :], s2.at[slot])

    def free3(slot):
        wait_bytes(tx3.at[slot, pl.ds(0, C - 1)], s3.at[slot])

    def free4(g, slot):
        wait_bytes(tx4.at[slot, pl.ds(0, Y * (R - 1))], s4.at[slot])
        own_copy(g, slot).wait()

    per = GI // CI

    def step(k, _):
        @pl.when(k + AHEAD < n)
        def _():
            send_row(k + AHEAD, 0, Y)

        @pl.when(k < n)
        def _():
            slot = lax.rem(k, SLOTS)
            rx1[k, :, my_y, :] = tx1[pl.ds(me_r * I + k * CI, CI), :, :]
            wait_bytes(rx1.at[k, :, pl.ds(0, Y * (R - 1)), :], r1.at[k])

            @pl.when(k >= SLOTS)
            def _():
                free2(slot)

            res = dot(b[...], jnp.concatenate([rx1[k, i] for i in range(CI)], axis=1)).astype(BF16)
            for i in range(CI):
                tx2[slot, i] = res[:, i * Z:(i + 1) * Z]
            for off in (2, 1, 3):
                p = col_peer(off)
                pltpu.make_async_remote_copy(
                    src_ref=tx2.at[slot, :, pl.ds(pl.multiple_of(p * J, J), J), :], dst_ref=rx2.at[k, me_c],
                    send_sem=s2.at[slot], recv_sem=r2.at[k], device_id={"col": p}, device_id_type=MESH).start()
            rx2[k, me_c] = tx2[slot, :, pl.ds(pl.multiple_of(me_c * J, J), J), :]

        m = k - LAG3

        @pl.when(jnp.logical_and(m >= 0, m < n))
        def _():
            slot = lax.rem(m, SLOTS)

            @pl.when(m + LAG3 + 2 < n)
            def _():
                load_d(m + LAG3 + 2).start()

            load_d(m).wait()
            wait_bytes(rx2.at[m, pl.ds(0, C - 1)], r2.at[m])

            @pl.when(m >= SLOTS)
            def _():
                free3(slot)

            lhs = jnp.concatenate([rx2[m, e].reshape(CI * J, Z) for e in range(C)], axis=1)
            h3 = (dot(lhs, ct[...]) * dbuf[slot].reshape(CI * J, N)).astype(BF16)
            h4 = dot(h3, c[...]).astype(BF16)
            for e in range(C):
                tx3[slot, e] = h4[:, e * Z:(e + 1) * Z].reshape(CI, J, Z)
            for off in (2, 1, 3):
                p = col_peer(off)
                pltpu.make_async_remote_copy(
                    src_ref=tx3.at[slot, p], dst_ref=rx3.at[m, :, pl.ds(pl.multiple_of(me_c * J, J), J), :],
                    send_sem=s3.at[slot], recv_sem=r3.at[m], device_id={"col": p}, device_id_type=MESH).start()
            rx3[m, :, pl.ds(pl.multiple_of(me_c * J, J), J), :] = tx3[slot, me_c]

        o = k - LAG5

        @pl.when(o >= 0)
        def _():
            wait_bytes(rx3.at[o, :, pl.ds(0, J * (C - 1)), :], r3.at[o])
            res = dot(bt[...], jnp.concatenate([rx3[o, i] for i in range(CI)], axis=1))
            g, q = lax.div(o, per), lax.rem(o, per)
            slot = lax.rem(g, 2)

            @pl.when(o < n - per)
            def _():
                for i in range(CI):
                    sa[0, pl.ds(q * CI + i, N, stride=GI), :] = res[:, i * Z:(i + 1) * Z]

            @pl.when(jnp.logical_and(o < n - per, q == per - 1))
            def _():
                @pl.when(g >= 2)
                def _():
                    free4(g - 2, slot)

                def pack(e, _):
                    y0 = e * 32
                    tx4[slot, pl.ds(y0, 32)] = (
                        sa[0, pl.ds(pl.multiple_of(y0 * GI, 32 * GI), 32 * GI), :].reshape(32, GI, Z).astype(BF16))
                    return 0

                lax.fori_loop(0, N // 32, pack, 0)
                for off in (4, 5, 3, 2, 6, 7, 1):
                    p = row_peer(off)
                    pltpu.make_async_remote_copy(
                        src_ref=tx4.at[slot, pl.ds(pl.multiple_of(p * Y, Y), Y)], dst_ref=to_h5(g),
                        send_sem=s4.at[slot], recv_sem=r4, device_id={"row": p}, device_id_type=MESH).start()
                own_copy(g, slot).start()

            @pl.when(o >= n - per)
            def _():
                for i in range(CI):
                    tx4b[q, i] = res[:, i * Z:(i + 1) * Z].astype(BF16)
                for off in (4, 5, 3, 2, 6, 7, 1):
                    p = row_peer(off)
                    pltpu.make_async_remote_copy(
                        src_ref=tx4b.at[q, :, pl.ds(pl.multiple_of(p * Y, Y), Y), :],
                        dst_ref=h5b.at[pl.ds(me_r * GI + q * CI, CI)],
                        send_sem=s5, recv_sem=r5, device_id={"row": p}, device_id_type=MESH).start()
                own_copy_b(q).start()

        @pl.when(k < Y // TY - 1)
        def _():
            second(k + 1)

        return 0

    lax.fori_loop(0, n + LAG5, step, 0)

    save_at.wait()
    wait_bytes(tx1.at[pl.ds(0, I * (R - 1))], s1)
    for m in range(n - SLOTS, n):
        free2(m % SLOTS)
        free3(m % SLOTS)
    groups = I // GI - 1
    for g in (groups - 2, groups - 1):
        free4(g, g % 2)
    for q in range(per):
        own_copy_b(q).wait()
    wait_bytes(tx4b.at[:, :, pl.ds(0, Y * (R - 1)), :], s5)
    wait_bytes(h5.at[:, pl.ds(0, keep * (R - 1)), :], r4)
    wait_bytes(h5b.at[pl.ds(0, GI * (R - 1))], r5)


def exchange(R, C, u, a, b, c, d):
    X, Y, Z = u.shape
    I, J, N = d.shape
    n = I // CI
    hb = pl.BlockSpec(memory_space=pl.ANY)
    DMA = pltpu.SemaphoreType.DMA
    return pl.pallas_call(
        functools.partial(exchange_kernel, R, C),
        name="exchange",
        out_shape=(jax.ShapeDtypeStruct((Y, N - R * GI, Z), BF16), jax.ShapeDtypeStruct((R * GI, Y, Z), BF16),
                   jax.ShapeDtypeStruct((X, N), BF16)),
        in_specs=[hb] * 5,
        out_specs=(hb, hb, hb),
        scratch_shapes=[
            pltpu.VMEM((6, N, X), BF16),
            pltpu.VMEM((2, X, TY, Z), BF16),
            pltpu.VMEM((Y // 8, X, 8 * Z), BF16),
            pltpu.VMEM((TY // 8, X * 8, Z), F32),
            pltpu.VMEM((TY // 8, N // 2 * 8, Z), F32),
            pltpu.VMEM((N, Y, Z), BF16),
            pltpu.VMEM((n, CI, N, Z), BF16),
            pltpu.VMEM((SLOTS, CI, N, Z), BF16),
            pltpu.VMEM((n, C, CI, J, Z), BF16),
            pltpu.VMEM((SLOTS, C, CI, J, Z), BF16),
            pltpu.VMEM((n, CI, N, Z), BF16),
            pltpu.VMEM((2, N, GI, Z), BF16),
            pltpu.VMEM((GI // CI, CI, N, Z), BF16),
            pltpu.VMEM((SLOTS, CI, J, N), F32),
            DMA((3,)), DMA((2,)), DMA((SLOTS,)), DMA, DMA((n,)), DMA((SLOTS,)), DMA((n,)), DMA((SLOTS,)), DMA((n,)),
            DMA((2,)), DMA, DMA((2,)), DMA, DMA, DMA((GI // CI,)), DMA,
        ],
        compiler_params=pltpu.CompilerParams(
            collective_id=0, has_side_effects=True, vmem_limit_bytes=67043328),
    )(u, a, b, c, d)


def last_kernel(at, h, hb, w, sc):
    T, K, Z = h.shape
    Kb, X = hb.shape[0], w.shape[0]
    sc[...] = hb[...].astype(F32).reshape(Kb * T, Z)
    rhs = jnp.concatenate(
        [jnp.concatenate([h[e], sc[pl.ds(e, Kb, stride=T), :].astype(BF16)], axis=0) for e in range(T)], axis=1)
    res = dot(at[...], rhs)
    flat = w.reshape(X * T, Z)
    for e in range(T):
        flat[pl.ds(e, X, stride=T), :] = res[:, e * Z:(e + 1) * Z]


def last(at, h, hb):
    Y, K, Z = h.shape
    Kb, X = hb.shape[0], at.shape[0]
    T = 8
    return pl.pallas_call(
        last_kernel,
        name="last",
        grid=(Y // T,),
        out_shape=jax.ShapeDtypeStruct((X, Y, Z), F32),
        in_specs=[pl.BlockSpec((X, K + Kb), lambda t: (0, 0)), pl.BlockSpec((T, K, Z), lambda t: (t, 0, 0)),
                  pl.BlockSpec((Kb, T, Z), lambda t: (0, t, 0))],
        out_specs=pl.BlockSpec((X, T, Z), lambda t: (0, t, 0)),
        scratch_shapes=[pltpu.VMEM((Kb * T, Z), F32)],
        compiler_params=pltpu.CompilerParams(vmem_limit_bytes=62 * 2**20),
    )(at, h, hb)


def solution(mesh):
    R, C = mesh.shape["row"], mesh.shape["col"]

    def local_apply(field_u, fac_a, fac_b, fac_c, diag_d):
        outs = []
        for e in range(field_u.shape[0]):
            h5, h5b, at = exchange(R, C, field_u[e], fac_a, fac_b, fac_c, diag_d)
            outs.append(last(at, h5, h5b))
        return jnp.stack(outs) if len(outs) > 1 else outs[0][None]

    spec = P("fields", None, "row", "col")
    fac = P("fields", None)
    return jax.shard_map(local_apply, mesh=mesh, in_specs=(spec, fac, fac, fac, P(("fields", "row"), "col", None)),
                         out_specs=spec, check_vma=False)
```

```python
import functools

import jax
import jax.numpy as jnp
from jax import lax
from jax.experimental import pallas as pl
from jax.experimental.pallas import tpu as pltpu
from jax.sharding import PartitionSpec as P

MESH = pl.DeviceIdType.MESH
F32, BF16 = jnp.float32, jnp.bfloat16
CI = 2
TY = 16
PITCH = 9
GI = 8
AHEAD = 4
EARLY = 2
LAG3, LAG5 = 1, 3
SLOTS = 4


def dot(a, b):
    return jnp.dot(a, b, preferred_element_type=F32)


def wait_bytes(ref, sem):
    pltpu.make_async_copy(ref, ref, sem).wait()


def exchange_kernel(R, C, u, a_hbm, b_hbm, c_hbm, d, h5, h5b, at_out, mats, ubuf, sa, sb, tx1, rx1, tx2, rx2, tx3, rx3,
                    tx4, tx4b, dbuf, msem, usem, dsem, s1, r1, s2, r2, s3, r3, s4, r4, s5, r5):
    X, Y, Z = u.shape
    I, J, N = d.shape
    n = I // CI
    a, b, c, bt, ct = (mats.at[e] for e in range(5))
    me_r, me_c = lax.axis_index("row"), lax.axis_index("col")

    def row_peer(off):
        return lax.rem(me_r + off, R)

    def col_peer(off):
        return lax.rem(me_c + off, C)

    def load_u(t):
        return pltpu.make_async_copy(u.at[:, pl.ds(t * TY, TY), :], ubuf.at[t % 2], usem.at[t % 2])

    def load_d(k):
        slot = lax.rem(k, SLOTS)
        return pltpu.make_async_copy(d.at[pl.ds(k * CI, CI)], dbuf.at[slot], dsem.at[slot])

    load_u(0).start()
    loads = [pltpu.make_async_copy(h, mats.at[e], msem.at[e]) for e, h in enumerate((a_hbm, b_hbm, c_hbm))]
    loads[0].start()
    load_u(1).start()
    for e in (1, 2):
        loads[e].start()

    barrier = pltpu.get_barrier_semaphore()
    for off in range(1, R):
        pl.semaphore_signal(barrier, inc=1, device_id={"row": row_peer(off)}, device_id_type=MESH)
    for off in range(1, C):
        pl.semaphore_signal(barrier, inc=1, device_id={"col": col_peer(off)}, device_id_type=MESH)

    def send_row(k, y0, ny):
        for off in range(1, R):
            p = row_peer(off)
            pltpu.make_async_remote_copy(
                src_ref=tx1.at[pl.ds(p * I + k * CI, CI), pl.ds(y0, ny), :],
                dst_ref=rx1.at[pl.ds(k * CI, CI), pl.ds(pl.multiple_of(me_r * Y + y0, TY), ny), :],
                send_sem=s1, recv_sem=r1.at[k], device_id={"row": p}, device_id_type=MESH).start()

    H = I // 2

    def project(half, h, rhs):
        res = dot(jnp.concatenate([a[pl.ds(e * I + half * H, H), :] for e in range(R)], axis=0), rhs)
        for e in range(8):
            sb[h, pl.ds(e, R * H, stride=PITCH), :] = res[:, e * Z:(e + 1) * Z]

    def gather(half, t):
        def body(e, _):
            for i in range(H):
                row = (e * H + i) * PITCH
                parts = [sb[h, pl.ds(row, 8), :] for h in range(TY // 8)]
                tx1[e * I + half * H + i, pl.ds(t * TY, TY), :] = jnp.concatenate(parts, axis=0).astype(BF16)
            return 0

        lax.fori_loop(0, R, body, 0)

    def kept(t, h, e):
        ref = rx3 if t < Y // TY // 2 else rx1
        return ref.at[I // 2 + (t % (Y // TY // 2)) * TY + h * 8 + e]

    def second(t):
        def body(h, _):
            project(1, h, jnp.concatenate([kept(t, h, e)[...] for e in range(8)], axis=1))
            return 0

        lax.fori_loop(0, TY // 8, body, 0)
        gather(1, t)

    for t in range(Y // TY):
        load_u(t).wait()
        slot = t % 2

        def spread(g, _):
            x0 = g * 32
            v = ubuf[slot, pl.ds(x0, 32)].astype(F32)
            for x in range(32):
                for h in range(TY // 8):
                    sa[h, pl.ds((x0 + x) * PITCH, 8), :] = v[x, h * 8:(h + 1) * 8, :]
            return 0

        lax.fori_loop(0, X // 32, spread, 0)
        if t + 2 < Y // TY:
            load_u(t + 2).start()
        if t == 0:
            loads[0].wait()

        def tile(h, _):
            cols = [sa[h, pl.ds(e, X, stride=PITCH), :].astype(BF16) for e in range(8)]
            for e in range(8):
                kept(t, h, e)[...] = cols[e]
            project(0, h, jnp.concatenate(cols, axis=1))
            return 0

        lax.fori_loop(0, TY // 8, tile, 0)
        gather(0, t)
        if t == 0:
            pl.semaphore_wait(barrier, R - 1 + C - 1)
        for k in range(EARLY):
            send_row(k, t * TY, TY)

    for k in range(EARLY, AHEAD):
        send_row(k, 0, Y)
    for k in range(LAG3 + 2):
        load_d(k).start()

    second(0)
    loads[1].wait()
    loads[2].wait()
    af = a[...].astype(F32)
    keep = I - GI
    order = [af[e * I:e * I + keep] for e in range(R)] + [af[e * I + keep:(e + 1) * I] for e in range(R)]
    at_out[...] = jnp.concatenate(order, axis=0).T.astype(BF16)
    for e in (1, 2):
        mats[2 + e] = mats[e].T

    my_y = pl.ds(pl.multiple_of(me_r * Y, Y), Y)

    def to_h5(g):
        return h5.at[:, pl.ds(pl.multiple_of(me_r * keep + g * GI, GI), GI), :]

    def free2(slot):
        wait_bytes(tx2.at[slot, :, pl.ds(0, J * (C - 1)), :], s2.at[slot])

    def free3(slot):
        wait_bytes(tx3.at[slot, pl.ds(0, C - 1)], s3.at[slot])

    def free4(g, slot):
        wait_bytes(tx4.at[slot, pl.ds(0, Y * (R - 1))], s4.at[slot])

    per = GI // CI

    def step(k, _):
        @pl.when(k + AHEAD < n)
        def _():
            send_row(k + AHEAD, 0, Y)

        @pl.when(k < n)
        def _():
            slot = lax.rem(k, SLOTS)
            rx1[pl.ds(k * CI, CI), my_y, :] = tx1[pl.ds(me_r * I + k * CI, CI), :, :]
            wait_bytes(rx1.at[pl.ds(0, CI), pl.ds(0, Y * (R - 1)), :], r1.at[k])

            @pl.when(k >= SLOTS)
            def _():
                free2(slot)

            res = dot(b[...], jnp.concatenate([rx1[k * CI + i] for i in range(CI)], axis=1)).astype(BF16)
            for i in range(CI):
                tx2[slot, i] = res[:, i * Z:(i + 1) * Z]
            for off in (2, 1, 3):
                p = col_peer(off)
                pltpu.make_async_remote_copy(
                    src_ref=tx2.at[slot, :, pl.ds(pl.multiple_of(p * J, J), J), :], dst_ref=rx2.at[k, me_c],
                    send_sem=s2.at[slot], recv_sem=r2.at[k], device_id={"col": p}, device_id_type=MESH).start()
            rx2[k, me_c] = tx2[slot, :, pl.ds(pl.multiple_of(me_c * J, J), J), :]

        m = k - LAG3

        @pl.when(jnp.logical_and(m >= 0, m < n))
        def _():
            slot = lax.rem(m, SLOTS)

            @pl.when(m + LAG3 + 2 < n)
            def _():
                load_d(m + LAG3 + 2).start()

            load_d(m).wait()
            wait_bytes(rx2.at[m, pl.ds(0, C - 1)], r2.at[m])

            @pl.when(m >= SLOTS)
            def _():
                free3(slot)

            lhs = jnp.concatenate([rx2[m, e].reshape(CI * J, Z) for e in range(C)], axis=1)
            h3 = (dot(lhs, ct[...]) * dbuf[slot].reshape(CI * J, N)).astype(BF16)
            h4 = dot(h3, c[...]).astype(BF16)
            for e in range(C):
                tx3[slot, e] = h4[:, e * Z:(e + 1) * Z].reshape(CI, J, Z)
            for off in (2, 1, 3):
                p = col_peer(off)
                pltpu.make_async_remote_copy(
                    src_ref=tx3.at[slot, p], dst_ref=rx3.at[pl.ds(m * CI, CI), pl.ds(pl.multiple_of(me_c * J, J), J), :],
                    send_sem=s3.at[slot], recv_sem=r3.at[m], device_id={"col": p}, device_id_type=MESH).start()
            rx3[pl.ds(m * CI, CI), pl.ds(pl.multiple_of(me_c * J, J), J), :] = tx3[slot, me_c]

        o = k - LAG5

        @pl.when(o >= 0)
        def _():
            wait_bytes(rx3.at[pl.ds(0, CI), pl.ds(0, J * (C - 1)), :], r3.at[o])
            res = dot(bt[...], jnp.concatenate([rx3[o * CI + i] for i in range(CI)], axis=1))
            g, q = lax.div(o, per), lax.rem(o, per)
            slot = lax.rem(g, 2)

            @pl.when(o < n - per)
            def _():
                for i in range(CI):
                    sa[0, pl.ds(q * CI + i, N, stride=GI), :] = res[:, i * Z:(i + 1) * Z]

            @pl.when(jnp.logical_and(o < n - per, q == per - 1))
            def _():
                @pl.when(g >= 2)
                def _():
                    free4(g - 2, slot)

                def pack(e, _):
                    y0 = e * 32
                    tx4[slot, pl.ds(y0, 32)] = (
                        sa[0, pl.ds(pl.multiple_of(y0 * GI, 32 * GI), 32 * GI), :].reshape(32, GI, Z).astype(BF16))
                    return 0

                lax.fori_loop(0, N // 32, pack, 0)
                for off in (4, 5, 3, 2, 6, 7, 1):
                    p = row_peer(off)
                    pltpu.make_async_remote_copy(
                        src_ref=tx4.at[slot, pl.ds(pl.multiple_of(p * Y, Y), Y)], dst_ref=to_h5(g),
                        send_sem=s4.at[slot], recv_sem=r4, device_id={"row": p}, device_id_type=MESH).start()
                to_h5(g)[...] = tx4[slot, my_y]

            @pl.when(o >= n - per)
            def _():
                for i in range(CI):
                    tx4b[q, i] = res[:, i * Z:(i + 1) * Z].astype(BF16)
                for off in (4, 5, 3, 2, 6, 7, 1):
                    p = row_peer(off)
                    pltpu.make_async_remote_copy(
                        src_ref=tx4b.at[q, :, pl.ds(pl.multiple_of(p * Y, Y), Y), :],
                        dst_ref=h5b.at[pl.ds(me_r * GI + q * CI, CI)],
                        send_sem=s5, recv_sem=r5, device_id={"row": p}, device_id_type=MESH).start()
                h5b[pl.ds(me_r * GI + q * CI, CI)] = tx4b[q, :, my_y, :]

        for t in range(1, Y // TY):
            pl.when(k == t - 1)(functools.partial(second, t))

        return 0

    lax.fori_loop(0, n + LAG5, step, 0)

    wait_bytes(tx1.at[pl.ds(0, I * (R - 1))], s1)
    for m in range(n - SLOTS, n):
        free2(m % SLOTS)
        free3(m % SLOTS)
    groups = I // GI - 1
    for g in (groups - 2, groups - 1):
        free4(g, g % 2)
    wait_bytes(tx4b.at[:, :, pl.ds(0, Y * (R - 1)), :], s5)
    wait_bytes(h5.at[:, pl.ds(0, keep * (R - 1)), :], r4)
    wait_bytes(h5b.at[pl.ds(0, GI * (R - 1))], r5)


def exchange(R, C, u, a, b, c, d):
    X, Y, Z = u.shape
    I, J, N = d.shape
    n = I // CI
    hb = pl.BlockSpec(memory_space=pl.ANY)
    vm = pl.BlockSpec(memory_space=pltpu.VMEM)
    DMA = pltpu.SemaphoreType.DMA
    return pl.pallas_call(
        functools.partial(exchange_kernel, R, C),
        name="exchange",
        out_shape=(pltpu.VMEM((Y, N - R * GI, Z), BF16), pltpu.VMEM((R * GI, Y, Z), BF16), pltpu.VMEM((X, N), BF16)),
        in_specs=[hb] * 5,
        out_specs=(vm, vm, vm),
        scratch_shapes=[
            pltpu.VMEM((5, N, X), BF16),
            pltpu.VMEM((2, X, TY, Z), BF16),
            pltpu.VMEM((TY // 8, X * PITCH, Z), F32),
            pltpu.VMEM((TY // 8, N // 2 * PITCH, Z), F32),
            pltpu.VMEM((N, Y, Z), BF16),
            pltpu.VMEM((I, N, Z), BF16),
            pltpu.VMEM((SLOTS, CI, N, Z), BF16),
            pltpu.VMEM((n, C, CI, J, Z), BF16),
            pltpu.VMEM((SLOTS, C, CI, J, Z), BF16),
            pltpu.VMEM((I, N, Z), BF16),
            pltpu.VMEM((2, N, GI, Z), BF16),
            pltpu.VMEM((GI // CI, CI, N, Z), BF16),
            pltpu.VMEM((SLOTS, CI, J, N), F32),
            DMA((3,)), DMA((2,)), DMA((SLOTS,)), DMA, DMA((n,)), DMA((SLOTS,)), DMA((n,)), DMA((SLOTS,)), DMA((n,)),
            DMA((2,)), DMA, DMA, DMA,
        ],
        compiler_params=pltpu.CompilerParams(
            collective_id=0, has_side_effects=True, vmem_limit_bytes=67043328 - 9 * 2**20),
    )(u, a, b, c, d)


def last_kernel(T, at, h, hb, w, sc):
    K, Z = h.shape[1:]
    Kb, X = hb.shape[0], w.shape[0]
    y0 = pl.multiple_of(pl.program_id(0) * T, T)
    sc[...] = hb[:, pl.ds(y0, T), :].astype(F32).reshape(Kb * T, Z)
    rhs = jnp.concatenate(
        [jnp.concatenate([h[y0 + e], sc[pl.ds(e, Kb, stride=T), :].astype(BF16)], axis=0) for e in range(T)], axis=1)
    res = dot(at[...], rhs)
    flat = w.reshape(X * T, Z)
    for e in range(T):
        flat[pl.ds(e, X, stride=T), :] = res[:, e * Z:(e + 1) * Z]


def last(at, h, hb):
    Y, K, Z = h.shape
    Kb, X = hb.shape[0], at.shape[0]
    T = 8
    vm = pl.BlockSpec(memory_space=pltpu.VMEM)
    inputs = [pltpu.with_memory_space_constraint(v, pltpu.VMEM) for v in (at, h, hb)]
    return pl.pallas_call(
        functools.partial(last_kernel, T),
        name="last",
        grid=(Y // T,),
        out_shape=jax.ShapeDtypeStruct((X, Y, Z), F32),
        in_specs=[vm, vm, vm],
        out_specs=pl.BlockSpec((X, T, Z), lambda t: (0, t, 0)),
        scratch_shapes=[pltpu.VMEM((Kb * T, Z), F32)],
        compiler_params=pltpu.CompilerParams(vmem_limit_bytes=32 * 2**20),
    )(*inputs)


def solution(mesh):
    R, C = mesh.shape["row"], mesh.shape["col"]

    def local_apply(field_u, fac_a, fac_b, fac_c, diag_d):
        outs = []
        for e in range(field_u.shape[0]):
            h5, h5b, at = exchange(R, C, field_u[e], fac_a, fac_b, fac_c, diag_d)
            outs.append(last(at, h5, h5b))
        return jnp.stack(outs) if len(outs) > 1 else outs[0][None]

    spec = P("fields", None, "row", "col")
    fac = P("fields", None)
    return jax.shard_map(local_apply, mesh=mesh, in_specs=(spec, fac, fac, fac, P(("fields", "row"), "col", None)),
                         out_specs=spec, check_vma=False)
```

```python
import functools

import jax
import jax.numpy as jnp
from jax import lax
from jax.experimental import pallas as pl
from jax.experimental.pallas import tpu as pltpu
from jax.sharding import PartitionSpec as P

MESH = pl.DeviceIdType.MESH
F32, BF16 = jnp.float32, jnp.bfloat16
CI = 2
TY = 16
PITCH = 9
GI = 8
AHEAD = 4
EARLY = 2
DPRE = 3
SLOTS = 4


def dot(a, b):
    return jnp.dot(a, b, preferred_element_type=F32)


def wait_bytes(ref, sem):
    pltpu.make_async_copy(ref, ref, sem).wait()


def exchange_kernel(R, C, u, a_hbm, b_hbm, c_hbm, d, h5, h5b, at_out, mats, ubuf, sa, sb, tx1, rx1, tx2, rx2, tx3, rx3,
                    tx4, tx4b, dbuf, msem, usem, dsem, s1, r1, s2, r2, s3, r3, s4, r4, s5, r5):
    X, Y, Z = u.shape
    I, J, N = d.shape
    n = I // CI
    a, b, c, bt, ct = (mats.at[e] for e in range(5))
    me_r, me_c = lax.axis_index("row"), lax.axis_index("col")

    def row_peer(off):
        return lax.rem(me_r + off, R)

    def col_peer(off):
        return lax.rem(me_c + off, C)

    def load_u(t):
        return pltpu.make_async_copy(u.at[:, pl.ds(t * TY, TY), :], ubuf.at[t % 2], usem.at[t % 2])

    def load_d(k):
        slot = lax.rem(k, SLOTS)
        return pltpu.make_async_copy(d.at[pl.ds(k * CI, CI)], dbuf.at[slot], dsem.at[slot])

    load_u(0).start()
    loads = [pltpu.make_async_copy(h, mats.at[e], msem.at[e]) for e, h in enumerate((a_hbm, b_hbm, c_hbm))]
    loads[0].start()
    load_u(1).start()
    for e in (1, 2):
        loads[e].start()

    barrier = pltpu.get_barrier_semaphore()
    for off in range(1, R):
        pl.semaphore_signal(barrier, inc=1, device_id={"row": row_peer(off)}, device_id_type=MESH)
    for off in range(1, C):
        pl.semaphore_signal(barrier, inc=1, device_id={"col": col_peer(off)}, device_id_type=MESH)

    def send_row(k, y0, ny):
        for off in range(1, R):
            p = row_peer(off)
            pltpu.make_async_remote_copy(
                src_ref=tx1.at[pl.ds(p * I + k * CI, CI), pl.ds(y0, ny), :],
                dst_ref=rx1.at[pl.ds(k * CI, CI), pl.ds(pl.multiple_of(me_r * Y + y0, TY), ny), :],
                send_sem=s1, recv_sem=r1.at[k], device_id={"row": p}, device_id_type=MESH).start()

    H = I // 2

    def project(half, h, rhs):
        res = dot(jnp.concatenate([a[pl.ds(e * I + half * H, H), :] for e in range(R)], axis=0), rhs)
        for e in range(8):
            sb[h, pl.ds(e, R * H, stride=PITCH), :] = res[:, e * Z:(e + 1) * Z]

    def gather(half, t):
        def body(e, _):
            for i in range(H):
                row = (e * H + i) * PITCH
                parts = [sb[h, pl.ds(row, 8), :] for h in range(TY // 8)]
                tx1[e * I + half * H + i, pl.ds(t * TY, TY), :] = jnp.concatenate(parts, axis=0).astype(BF16)
            return 0

        lax.fori_loop(0, R, body, 0)

    def kept(t, h, e):
        ref = rx3 if t < Y // TY // 2 else rx1
        return ref.at[I // 2 + (t % (Y // TY // 2)) * TY + h * 8 + e]

    def second(t):
        def body(h, _):
            project(1, h, jnp.concatenate([kept(t, h, e)[...] for e in range(8)], axis=1))
            return 0

        lax.fori_loop(0, TY // 8, body, 0)
        gather(1, t)

    for t in range(Y // TY):
        load_u(t).wait()
        slot = t % 2

        def spread(g, _):
            x0 = g * 32
            v = ubuf[slot, pl.ds(x0, 32)].astype(F32)
            for x in range(32):
                for h in range(TY // 8):
                    sa[h, pl.ds((x0 + x) * PITCH, 8), :] = v[x, h * 8:(h + 1) * 8, :]
            return 0

        lax.fori_loop(0, X // 32, spread, 0)
        if t + 2 < Y // TY:
            load_u(t + 2).start()
        if t == 0:
            loads[0].wait()

        def tile(h, _):
            cols = [sa[h, pl.ds(e, X, stride=PITCH), :].astype(BF16) for e in range(8)]
            for e in range(8):
                kept(t, h, e)[...] = cols[e]
            project(0, h, jnp.concatenate(cols, axis=1))
            return 0

        lax.fori_loop(0, TY // 8, tile, 0)
        gather(0, t)
        if t == 0:
            pl.semaphore_wait(barrier, R - 1 + C - 1)
        for k in range(EARLY):
            send_row(k, t * TY, TY)

    for k in range(EARLY, AHEAD):
        send_row(k, 0, Y)
    for k in range(DPRE):
        load_d(k).start()

    second(0)
    loads[1].wait()
    loads[2].wait()
    af = a[...].astype(F32)
    keep = I - GI
    order = [af[e * I:e * I + keep] for e in range(R)] + [af[e * I + keep:(e + 1) * I] for e in range(R)]
    at_out[...] = jnp.concatenate(order, axis=0).T.astype(BF16)
    for e in (1, 2):
        mats[2 + e] = mats[e].T

    my_y = pl.ds(pl.multiple_of(me_r * Y, Y), Y)

    def to_h5(g):
        return h5.at[:, pl.ds(pl.multiple_of(me_r * keep + g * GI, GI), GI), :]

    def free2(slot):
        wait_bytes(tx2.at[slot, :, pl.ds(0, J * (C - 1)), :], s2.at[slot])

    def free3(slot):
        wait_bytes(tx3.at[slot, pl.ds(0, C - 1)], s3.at[slot])

    def free4(g, slot):
        wait_bytes(tx4.at[slot, pl.ds(0, Y * (R - 1))], s4.at[slot])

    per = GI // CI

    def step(k, _):
        @pl.when(k + AHEAD < n)
        def _():
            send_row(k + AHEAD, 0, Y)

        @pl.when(k < n)
        def _():
            slot = lax.rem(k, SLOTS)
            rx1[pl.ds(k * CI, CI), my_y, :] = tx1[pl.ds(me_r * I + k * CI, CI), :, :]
            wait_bytes(rx1.at[pl.ds(0, CI), pl.ds(0, Y * (R - 1)), :], r1.at[k])

            @pl.when(k >= SLOTS)
            def _():
                free2(slot)

            res = dot(b[...], jnp.concatenate([rx1[k * CI + i] for i in range(CI)], axis=1)).astype(BF16)
            for i in range(CI):
                tx2[slot, i] = res[:, i * Z:(i + 1) * Z]
            for off in (2, 1, 3):
                p = col_peer(off)
                pltpu.make_async_remote_copy(
                    src_ref=tx2.at[slot, :, pl.ds(pl.multiple_of(p * J, J), J), :], dst_ref=rx2.at[k, me_c],
                    send_sem=s2.at[slot], recv_sem=r2.at[k], device_id={"col": p}, device_id_type=MESH).start()
            rx2[k, me_c] = tx2[slot, :, pl.ds(pl.multiple_of(me_c * J, J), J), :]

        def middle(m, _):
            slot = lax.rem(m, SLOTS)

            @pl.when(m + DPRE < n)
            def _():
                load_d(m + DPRE).start()

            load_d(m).wait()
            wait_bytes(rx2.at[m, pl.ds(0, C - 1)], r2.at[m])

            @pl.when(m >= SLOTS)
            def _():
                free3(slot)

            lhs = jnp.concatenate([rx2[m, e].reshape(CI * J, Z) for e in range(C)], axis=1)
            h3 = (dot(lhs, ct[...]) * dbuf[slot].reshape(CI * J, N)).astype(BF16)
            h4 = dot(h3, c[...]).astype(BF16)
            for e in range(C):
                tx3[slot, e] = h4[:, e * Z:(e + 1) * Z].reshape(CI, J, Z)
            for off in (2, 1, 3):
                p = col_peer(off)
                pltpu.make_async_remote_copy(
                    src_ref=tx3.at[slot, p], dst_ref=rx3.at[pl.ds(m * CI, CI), pl.ds(pl.multiple_of(me_c * J, J), J), :],
                    send_sem=s3.at[slot], recv_sem=r3.at[m], device_id={"col": p}, device_id_type=MESH).start()
            rx3[pl.ds(m * CI, CI), pl.ds(pl.multiple_of(me_c * J, J), J), :] = tx3[slot, me_c]
            return 0

        turn = n // 2
        lo = jnp.maximum(jnp.where(k <= turn, k - 2, k - 1), 0)
        hi = jnp.minimum(jnp.where(k < turn, k - 1, k), n)
        lax.fori_loop(lo, hi, middle, 0)

        def late(o, _):
            wait_bytes(rx3.at[pl.ds(0, CI), pl.ds(0, J * (C - 1)), :], r3.at[o])
            res = dot(bt[...], jnp.concatenate([rx3[o * CI + i] for i in range(CI)], axis=1))
            g, q = lax.div(o, per), lax.rem(o, per)
            slot = lax.rem(g, 2)

            @pl.when(o < n - per)
            def _():
                for i in range(CI):
                    sa[0, pl.ds(q * CI + i, N, stride=GI), :] = res[:, i * Z:(i + 1) * Z]

            @pl.when(jnp.logical_and(o < n - per, q == per - 1))
            def _():
                @pl.when(g >= 2)
                def _():
                    free4(g - 2, slot)

                def pack(e, _):
                    y0 = e * 32
                    tx4[slot, pl.ds(y0, 32)] = (
                        sa[0, pl.ds(pl.multiple_of(y0 * GI, 32 * GI), 32 * GI), :].reshape(32, GI, Z).astype(BF16))
                    return 0

                lax.fori_loop(0, N // 32, pack, 0)
                for off in (4, 5, 3, 2, 6, 7, 1):
                    p = row_peer(off)
                    pltpu.make_async_remote_copy(
                        src_ref=tx4.at[slot, pl.ds(pl.multiple_of(p * Y, Y), Y)], dst_ref=to_h5(g),
                        send_sem=s4.at[slot], recv_sem=r4, device_id={"row": p}, device_id_type=MESH).start()
                to_h5(g)[...] = tx4[slot, my_y]

            @pl.when(o >= n - per)
            def _():
                for i in range(CI):
                    tx4b[q, i] = res[:, i * Z:(i + 1) * Z].astype(BF16)
                for off in (4, 5, 3, 2, 6, 7, 1):
                    p = row_peer(off)
                    pltpu.make_async_remote_copy(
                        src_ref=tx4b.at[q, :, pl.ds(pl.multiple_of(p * Y, Y), Y), :],
                        dst_ref=h5b.at[pl.ds(me_r * GI + q * CI, CI)],
                        send_sem=s5, recv_sem=r5, device_id={"row": p}, device_id_type=MESH).start()
                h5b[pl.ds(me_r * GI + q * CI, CI)] = tx4b[q, :, my_y, :]
            return 0

        lo5 = jnp.maximum(jnp.where(k <= turn + 1, k - 3, k - 2), 0)
        hi5 = jnp.minimum(jnp.where(k < turn + 1, k - 2, k - 1), n)
        lax.fori_loop(lo5, hi5, late, 0)

        for t in range(1, Y // TY):
            pl.when(k == t - 1)(functools.partial(second, t))

        return 0

    lax.fori_loop(0, n + 2, step, 0)

    wait_bytes(tx1.at[pl.ds(0, I * (R - 1))], s1)
    for m in range(n - SLOTS, n):
        free2(m % SLOTS)
        free3(m % SLOTS)
    groups = I // GI - 1
    for g in (groups - 2, groups - 1):
        free4(g, g % 2)
    wait_bytes(tx4b.at[:, :, pl.ds(0, Y * (R - 1)), :], s5)
    wait_bytes(h5.at[:, pl.ds(0, keep * (R - 1)), :], r4)
    wait_bytes(h5b.at[pl.ds(0, GI * (R - 1))], r5)


def exchange(R, C, u, a, b, c, d):
    X, Y, Z = u.shape
    I, J, N = d.shape
    n = I // CI
    hb = pl.BlockSpec(memory_space=pl.ANY)
    vm = pl.BlockSpec(memory_space=pltpu.VMEM)
    DMA = pltpu.SemaphoreType.DMA
    return pl.pallas_call(
        functools.partial(exchange_kernel, R, C),
        name="exchange",
        out_shape=(pltpu.VMEM((Y, N - R * GI, Z), BF16), pltpu.VMEM((R * GI, Y, Z), BF16), pltpu.VMEM((X, N), BF16)),
        in_specs=[hb] * 5,
        out_specs=(vm, vm, vm),
        scratch_shapes=[
            pltpu.VMEM((5, N, X), BF16),
            pltpu.VMEM((2, X, TY, Z), BF16),
            pltpu.VMEM((TY // 8, X * PITCH, Z), F32),
            pltpu.VMEM((TY // 8, N // 2 * PITCH, Z), F32),
            pltpu.VMEM((N, Y, Z), BF16),
            pltpu.VMEM((I, N, Z), BF16),
            pltpu.VMEM((SLOTS, CI, N, Z), BF16),
            pltpu.VMEM((n, C, CI, J, Z), BF16),
            pltpu.VMEM((SLOTS, C, CI, J, Z), BF16),
            pltpu.VMEM((I, N, Z), BF16),
            pltpu.VMEM((2, N, GI, Z), BF16),
            pltpu.VMEM((GI // CI, CI, N, Z), BF16),
            pltpu.VMEM((SLOTS, CI, J, N), F32),
            DMA((3,)), DMA((2,)), DMA((SLOTS,)), DMA, DMA((n,)), DMA((SLOTS,)), DMA((n,)), DMA((SLOTS,)), DMA((n,)),
            DMA((2,)), DMA, DMA, DMA,
        ],
        compiler_params=pltpu.CompilerParams(
            collective_id=0, has_side_effects=True, vmem_limit_bytes=67043328 - 9 * 2**20),
    )(u, a, b, c, d)


def last_kernel(T, at, h, hb, w, sc):
    K, Z = h.shape[1:]
    Kb, X = hb.shape[0], w.shape[0]
    y0 = pl.multiple_of(pl.program_id(0) * T, T)
    sc[...] = hb[:, pl.ds(y0, T), :].astype(F32).reshape(Kb * T, Z)
    rhs = jnp.concatenate(
        [jnp.concatenate([h[y0 + e], sc[pl.ds(e, Kb, stride=T), :].astype(BF16)], axis=0) for e in range(T)], axis=1)
    res = dot(at[...], rhs)
    flat = w.reshape(X * T, Z)
    for e in range(T):
        flat[pl.ds(e, X, stride=T), :] = res[:, e * Z:(e + 1) * Z]


def last(at, h, hb):
    Y, K, Z = h.shape
    Kb, X = hb.shape[0], at.shape[0]
    T = 8
    vm = pl.BlockSpec(memory_space=pltpu.VMEM)
    inputs = [pltpu.with_memory_space_constraint(v, pltpu.VMEM) for v in (at, h, hb)]
    return pl.pallas_call(
        functools.partial(last_kernel, T),
        name="last",
        grid=(Y // T,),
        out_shape=jax.ShapeDtypeStruct((X, Y, Z), F32),
        in_specs=[vm, vm, vm],
        out_specs=pl.BlockSpec((X, T, Z), lambda t: (0, t, 0)),
        scratch_shapes=[pltpu.VMEM((Kb * T, Z), F32)],
        compiler_params=pltpu.CompilerParams(vmem_limit_bytes=32 * 2**20),
    )(*inputs)


def solution(mesh):
    R, C = mesh.shape["row"], mesh.shape["col"]

    def local_apply(field_u, fac_a, fac_b, fac_c, diag_d):
        outs = []
        for e in range(field_u.shape[0]):
            h5, h5b, at = exchange(R, C, field_u[e], fac_a, fac_b, fac_c, diag_d)
            outs.append(last(at, h5, h5b))
        return jnp.stack(outs) if len(outs) > 1 else outs[0][None]

    spec = P("fields", None, "row", "col")
    fac = P("fields", None)
    return jax.shard_map(local_apply, mesh=mesh, in_specs=(spec, fac, fac, fac, P(("fields", "row"), "col", None)),
                         out_specs=spec, check_vma=False)
```

```python
import functools

import jax
import jax.numpy as jnp
from jax import lax
from jax.experimental import pallas as pl
from jax.experimental.pallas import tpu as pltpu
from jax.sharding import PartitionSpec as P

MESH = pl.DeviceIdType.MESH
F32, BF16 = jnp.float32, jnp.bfloat16
CI = 2
TY = 16
PITCH = 9
GI = 8
AHEAD = 4
EARLY = 1
DPRE = 3
LAG0, LAG1, LAG5 = 2, 1, 1
XPARTS = 2
BUFS = 3
SLOTS = 4


def dot(a, b):
    return jnp.dot(a, b, preferred_element_type=F32)


def wait_bytes(ref, sem):
    pltpu.make_async_copy(ref, ref, sem).wait()


def exchange_kernel(R, C, u, a_hbm, b_hbm, c_hbm, d, h5, h5b, at_out, mats, ubuf, sa, sb, tx1, rx1, tx2, rx2, tx3, rx3,
                    tx4, tx4b, dbuf, msem, usem, dsem, s1, r1, s2, r2, s3, r3, s4, r4, s5, r5):
    X, Y, Z = u.shape
    I, J, N = d.shape
    n = I // CI
    a, b, c, bt, ct = (mats.at[e] for e in range(5))
    me_r, me_c = lax.axis_index("row"), lax.axis_index("col")

    def row_peer(off):
        return lax.rem(me_r + off, R)

    def col_peer(off):
        return lax.rem(me_c + off, C)

    def load_u(t):
        return pltpu.make_async_copy(u.at[:, pl.ds(t * TY, TY), :], ubuf.at[t % 2], usem.at[t % 2])

    def load_d(k):
        slot = lax.rem(k, SLOTS)
        return pltpu.make_async_copy(d.at[pl.ds(k * CI, CI)], dbuf.at[slot], dsem.at[slot])

    load_u(0).start()
    loads = [pltpu.make_async_copy(h, mats.at[e], msem.at[e]) for e, h in enumerate((a_hbm, b_hbm, c_hbm))]
    loads[0].start()
    load_u(1).start()
    for e in (1, 2):
        loads[e].start()

    barrier = pltpu.get_barrier_semaphore()
    for off in range(1, R):
        pl.semaphore_signal(barrier, inc=1, device_id={"row": row_peer(off)}, device_id_type=MESH)
    for off in range(1, C):
        pl.semaphore_signal(barrier, inc=1, device_id={"col": col_peer(off)}, device_id_type=MESH)

    def send_row(k, y0, ny):
        for off in range(1, R):
            p = row_peer(off)
            pltpu.make_async_remote_copy(
                src_ref=tx1.at[pl.ds(p * I + k * CI, CI), pl.ds(y0, ny), :],
                dst_ref=rx1.at[pl.ds(k * CI, CI), pl.ds(pl.multiple_of(me_r * Y + y0, TY), ny), :],
                send_sem=s1, recv_sem=r1.at[k], device_id={"row": p}, device_id_type=MESH).start()

    H = I // 2

    def project(half, h, rhs):
        res = dot(jnp.concatenate([a[pl.ds(e * I + half * H, H), :] for e in range(R)], axis=0), rhs)
        for e in range(8):
            sb[h, pl.ds(e, R * H, stride=PITCH), :] = res[:, e * Z:(e + 1) * Z]

    def gather(half, t):
        def body(e, _):
            for i in range(H):
                row = (e * H + i) * PITCH
                parts = [sb[h, pl.ds(row, 8), :] for h in range(TY // 8)]
                tx1[e * I + half * H + i, pl.ds(t * TY, TY), :] = jnp.concatenate(parts, axis=0).astype(BF16)
            return 0

        lax.fori_loop(0, R, body, 0)

    def kept(t, h, e):
        ref = rx3 if t < Y // TY // 2 else rx1
        return ref.at[I // 2 + (t % (Y // TY // 2)) * TY + h * 8 + e]

    def second(t):
        def body(h, _):
            project(1, h, jnp.concatenate([kept(t, h, e)[...] for e in range(8)], axis=1))
            return 0

        lax.fori_loop(0, TY // 8, body, 0)
        gather(1, t)

    for t in range(Y // TY):
        load_u(t).wait()
        slot = t % 2

        def spread(g, _):
            x0 = g * 32
            v = ubuf[slot, pl.ds(x0, 32)].astype(F32)
            for x in range(32):
                for h in range(TY // 8):
                    sa[h, pl.ds((x0 + x) * PITCH, 8), :] = v[x, h * 8:(h + 1) * 8, :]
            return 0

        lax.fori_loop(0, X // 32, spread, 0)
        if t + 2 < Y // TY:
            load_u(t + 2).start()
        if t == 0:
            loads[0].wait()

        def tile(h, _):
            cols = [sa[h, pl.ds(e, X, stride=PITCH), :].astype(BF16) for e in range(8)]
            for e in range(8):
                kept(t, h, e)[...] = cols[e]
            project(0, h, jnp.concatenate(cols, axis=1))
            return 0

        lax.fori_loop(0, TY // 8, tile, 0)
        gather(0, t)
        if t == 0:
            pl.semaphore_wait(barrier, R - 1 + C - 1)
        for k in range(EARLY):
            send_row(k, t * TY, TY)

    for k in range(EARLY, AHEAD):
        send_row(k, 0, Y)
    for k in range(DPRE):
        load_d(k).start()

    second(0)
    loads[1].wait()
    loads[2].wait()
    af = a[...].astype(F32)
    keep = I - GI
    order = [af[e * I:e * I + keep] for e in range(R)] + [af[e * I + keep:(e + 1) * I] for e in range(R)]
    at_out[...] = jnp.concatenate(order, axis=0).T.astype(BF16)
    for e in (1, 2):
        mats[2 + e] = mats[e].T

    my_y = pl.ds(pl.multiple_of(me_r * Y, Y), Y)

    def to_h5(g):
        return h5.at[:, pl.ds(pl.multiple_of(me_r * keep + g * GI, GI), GI), :]

    def free2(slot):
        wait_bytes(tx2.at[slot, :, pl.ds(0, J * (C - 1)), :], s2.at[slot])

    def free3(slot):
        wait_bytes(tx3.at[slot, pl.ds(0, C - 1)], s3.at[slot])

    def free4(g, slot):
        wait_bytes(tx4.at[slot, pl.ds(0, Y * (R - 1))], s4.at[slot])

    per = GI // CI

    def step(k, _):
        @pl.when(k + AHEAD < n)
        def _():
            send_row(k + AHEAD, 0, Y)

        @pl.when(k < n)
        def _():
            slot = lax.rem(k, SLOTS)
            rx1[pl.ds(k * CI, CI), my_y, :] = tx1[pl.ds(me_r * I + k * CI, CI), :, :]
            wait_bytes(rx1.at[pl.ds(0, CI), pl.ds(0, Y * (R - 1)), :], r1.at[k])

            @pl.when(k >= SLOTS)
            def _():
                free2(slot)

            res = dot(b[...], jnp.concatenate([rx1[k * CI + i] for i in range(CI)], axis=1)).astype(BF16)
            for i in range(CI):
                tx2[slot, i] = res[:, i * Z:(i + 1) * Z]
            for off in (2, 1, 3):
                p = col_peer(off)
                pltpu.make_async_remote_copy(
                    src_ref=tx2.at[slot, :, pl.ds(pl.multiple_of(p * J, J), J), :], dst_ref=rx2.at[k, me_c],
                    send_sem=s2.at[slot], recv_sem=r2.at[k], device_id={"col": p}, device_id_type=MESH).start()
            rx2[k, me_c] = tx2[slot, :, pl.ds(pl.multiple_of(me_c * J, J), J), :]

        def middle(m, _):
            slot = lax.rem(m, SLOTS)

            @pl.when(m + DPRE < n)
            def _():
                load_d(m + DPRE).start()

            load_d(m).wait()
            wait_bytes(rx2.at[m, pl.ds(0, C - 1)], r2.at[m])

            @pl.when(m >= SLOTS)
            def _():
                free3(slot)

            lhs = jnp.concatenate([rx2[m, e].reshape(CI * J, Z) for e in range(C)], axis=1)
            h3 = (dot(lhs, ct[...]) * dbuf[slot].reshape(CI * J, N)).astype(BF16)
            h4 = dot(h3, c[...]).astype(BF16)
            for e in range(C):
                tx3[slot, e] = h4[:, e * Z:(e + 1) * Z].reshape(CI, J, Z)
            for i in range(CI):
                for off in (2, 1, 3):
                    p = col_peer(off)
                    pltpu.make_async_remote_copy(
                        src_ref=tx3.at[slot, p, i], dst_ref=rx3.at[m * CI + i, pl.ds(pl.multiple_of(me_c * J, J), J), :],
                        send_sem=s3.at[slot], recv_sem=r3.at[m * CI + i], device_id={"col": p}, device_id_type=MESH).start()
            rx3[pl.ds(m * CI, CI), pl.ds(pl.multiple_of(me_c * J, J), J), :] = tx3[slot, me_c]
            return 0

        turn = n // 2
        lo = jnp.maximum(jnp.where(k <= turn, k - LAG0, k - LAG1), 0)
        hi = jnp.minimum(jnp.where(k < turn, k - LAG0, k - LAG1) + 1, n)
        lax.fori_loop(lo, hi, middle, 0)

        def late(o, _):
            g, q = lax.div(o, per), lax.rem(o, per)
            slot = lax.rem(g, 2)

            def arrived(i):
                wait_bytes(rx3.at[0, pl.ds(0, J * (C - 1)), :], r3.at[o * CI + i])

            @pl.when(o < n - per)
            def _():
                for i in range(CI):
                    arrived(i)
                res = dot(bt[...], jnp.concatenate([rx3[o * CI + i] for i in range(CI)], axis=1))
                for i in range(CI):
                    sa[0, pl.ds(q * CI + i, N, stride=GI), :] = res[:, i * Z:(i + 1) * Z]

            @pl.when(jnp.logical_and(o < n - per, q == per - 1))
            def _():
                @pl.when(g >= 2)
                def _():
                    free4(g - 2, slot)

                def pack(e, _):
                    y0 = e * 32
                    tx4[slot, pl.ds(y0, 32)] = (
                        sa[0, pl.ds(pl.multiple_of(y0 * GI, 32 * GI), 32 * GI), :].reshape(32, GI, Z).astype(BF16))
                    return 0

                lax.fori_loop(0, N // 32, pack, 0)
                for off in (4, 5, 3, 2, 6, 7, 1):
                    p = row_peer(off)
                    pltpu.make_async_remote_copy(
                        src_ref=tx4.at[slot, pl.ds(pl.multiple_of(p * Y, Y), Y)], dst_ref=to_h5(g),
                        send_sem=s4.at[slot], recv_sem=r4, device_id={"row": p}, device_id_type=MESH).start()
                to_h5(g)[...] = tx4[slot, my_y]

            @pl.when(o >= n - per)
            def _():
                for i in range(CI):
                    arrived(i)
                    tx4b[q, i] = dot(bt[...], rx3[o * CI + i]).astype(BF16)
                    row = me_r * GI + q * CI + i
                    for off in (4, 5, 3, 2, 6, 7, 1):
                        p = row_peer(off)
                        pltpu.make_async_remote_copy(
                            src_ref=tx4b.at[q, i, pl.ds(pl.multiple_of(p * Y, Y), Y), :], dst_ref=h5b.at[row],
                            send_sem=s5, recv_sem=r5, device_id={"row": p}, device_id_type=MESH).start()
                    h5b[row] = tx4b[q, i, my_y, :]
            return 0

        lo5 = jnp.maximum(jnp.where(k <= turn, k - LAG0, k - LAG1) - LAG5, 0)
        hi5 = jnp.minimum(jnp.where(k < turn, k - LAG0, k - LAG1) - LAG5 + 1, n)
        lax.fori_loop(lo5, hi5, late, 0)

        for t in range(1, Y // TY):
            pl.when(k == t - 1)(functools.partial(second, t))

        return 0

    lax.fori_loop(0, n + LAG1 + LAG5, step, 0)

    wait_bytes(tx1.at[pl.ds(0, I * (R - 1))], s1)
    for m in range(n - SLOTS, n):
        free2(m % SLOTS)
        free3(m % SLOTS)
    groups = I // GI - 1
    for g in (groups - 2, groups - 1):
        free4(g, g % 2)
    wait_bytes(tx4b.at[:, :, pl.ds(0, Y * (R - 1)), :], s5)
    wait_bytes(h5.at[:, pl.ds(0, keep * (R - 1)), :], r4)
    wait_bytes(h5b.at[pl.ds(0, GI * (R - 1))], r5)


def exchange(R, C, u, a, b, c, d):
    X, Y, Z = u.shape
    I, J, N = d.shape
    n = I // CI
    hb = pl.BlockSpec(memory_space=pl.ANY)
    vm = pl.BlockSpec(memory_space=pltpu.VMEM)
    DMA = pltpu.SemaphoreType.DMA
    return pl.pallas_call(
        functools.partial(exchange_kernel, R, C),
        name="exchange",
        out_shape=(pltpu.VMEM((Y, N - R * GI, Z), BF16), pltpu.VMEM((R * GI, Y, Z), BF16), pltpu.VMEM((X, N), BF16)),
        in_specs=[hb] * 5,
        out_specs=(vm, vm, vm),
        scratch_shapes=[
            pltpu.VMEM((5, N, X), BF16),
            pltpu.VMEM((2, X, TY, Z), BF16),
            pltpu.VMEM((TY // 8, X * PITCH, Z), F32),
            pltpu.VMEM((TY // 8, N // 2 * PITCH, Z), F32),
            pltpu.VMEM((N, Y, Z), BF16),
            pltpu.VMEM((I, N, Z), BF16),
            pltpu.VMEM((SLOTS, CI, N, Z), BF16),
            pltpu.VMEM((n, C, CI, J, Z), BF16),
            pltpu.VMEM((SLOTS, C, CI, J, Z), BF16),
            pltpu.VMEM((I, N, Z), BF16),
            pltpu.VMEM((2, N, GI, Z), BF16),
            pltpu.VMEM((GI // CI, CI, N, Z), BF16),
            pltpu.VMEM((SLOTS, CI, J, N), F32),
            DMA((3,)), DMA((2,)), DMA((SLOTS,)), DMA, DMA((n,)), DMA((SLOTS,)), DMA((n,)), DMA((SLOTS,)), DMA((I,)),
            DMA((2,)), DMA, DMA, DMA,
        ],
        compiler_params=pltpu.CompilerParams(
            collective_id=0, has_side_effects=True, vmem_limit_bytes=67043328 - 9 * 2**20),
    )(u, a, b, c, d)


def last_kernel(at, h, hb, w, buf, sc, sem):
    Y, K, Z = h.shape
    Kb, X = hb.shape[0], w.shape[0]
    XB = X // XPARTS
    T = buf.shape[2]
    copies = []
    for t in range(Y // T):
        slot = t % BUFS
        if t >= BUFS:
            for copy in copies[t - BUFS]:
                copy.wait()
        sc[...] = hb[:, t * T:(t + 1) * T, :].astype(F32).reshape(Kb * T, Z)
        rhs = jnp.concatenate(
            [jnp.concatenate([h[t * T + e], sc[pl.ds(e, Kb, stride=T), :].astype(BF16)], axis=0) for e in range(T)], axis=1)
        flat = buf.at[slot].reshape(X * T, Z)
        copies.append([])
        for m in range(XPARTS):
            res = dot(at[m * XB:(m + 1) * XB, :], rhs)
            for e in range(T):
                flat[pl.ds(m * XB * T + e, XB, stride=T), :] = res[:, e * Z:(e + 1) * Z]
            copy = pltpu.make_async_copy(
                buf.at[slot, pl.ds(m * XB, XB)], w.at[pl.ds(m * XB, XB), pl.ds(t * T, T), :], sem.at[slot, m])
            copy.start()
            copies[t].append(copy)
    for t in range(Y // T - BUFS, Y // T):
        for copy in copies[t]:
            copy.wait()


def last(at, h, hb):
    Y, K, Z = h.shape
    Kb, X = hb.shape[0], at.shape[0]
    T = 8
    vm = pl.BlockSpec(memory_space=pltpu.VMEM)
    inputs = [pltpu.with_memory_space_constraint(v, pltpu.VMEM) for v in (at, h, hb)]
    return pl.pallas_call(
        last_kernel,
        name="last",
        out_shape=jax.ShapeDtypeStruct((X, Y, Z), F32),
        in_specs=[vm, vm, vm],
        out_specs=pl.BlockSpec(memory_space=pl.ANY),
        scratch_shapes=[pltpu.VMEM((BUFS, X, T, Z), F32), pltpu.VMEM((Kb * T, Z), F32),
                        pltpu.SemaphoreType.DMA((BUFS, XPARTS))],
        compiler_params=pltpu.CompilerParams(vmem_limit_bytes=40 * 2**20),
    )(*inputs)


def solution(mesh):
    R, C = mesh.shape["row"], mesh.shape["col"]

    def local_apply(field_u, fac_a, fac_b, fac_c, diag_d):
        outs = []
        for e in range(field_u.shape[0]):
            h5, h5b, at = exchange(R, C, field_u[e], fac_a, fac_b, fac_c, diag_d)
            outs.append(last(at, h5, h5b))
        return jnp.stack(outs) if len(outs) > 1 else outs[0][None]

    spec = P("fields", None, "row", "col")
    fac = P("fields", None)
    return jax.shard_map(local_apply, mesh=mesh, in_specs=(spec, fac, fac, fac, P(("fields", "row"), "col", None)),
                         out_specs=spec, check_vma=False)
```

```python
import functools

import jax
import jax.numpy as jnp
from jax import lax
from jax.experimental import pallas as pl
from jax.experimental.pallas import tpu as pltpu
from jax.sharding import PartitionSpec as P

MESH = pl.DeviceIdType.MESH
F32, BF16 = jnp.float32, jnp.bfloat16
CI = 2
TY = 16
PITCH = 9
GI = 8
AHEAD = 4
EARLY = 1
DPRE = 3
LAG0, LAG1, LAG5 = 2, 1, 1
XPARTS = 2
BUFS = 3
SLOTS = 4
RING1, RING = 16, 8
PARTS = 4


def dot(a, b):
    return jnp.dot(a, b, preferred_element_type=F32)


def wait_bytes(ref, sem):
    pltpu.make_async_copy(ref, ref, sem).wait()


def exchange_kernel(R, C, u, a_hbm, b_hbm, c_hbm, d, h5, h5b, at_out, mats, ubuf, sa, sb, tx1, rx1, tx2, rx2, tx3, rx3,
                    tx4, tx4b, dbuf, msem, usem, dsem, s1, r1, s2, r2, s3, r3, s4, r4, s5, r5):
    X, Y, Z = u.shape
    I, J, N = d.shape
    n = I // CI
    a, b, c, bt, ct = (mats.at[e] for e in range(5))
    me_r, me_c = lax.axis_index("row"), lax.axis_index("col")

    def row_peer(off):
        return lax.rem(me_r + off, R)

    def col_peer(off):
        return lax.rem(me_c + off, C)

    def load_u(t):
        return pltpu.make_async_copy(u.at[:, pl.ds(t * TY, TY), :], ubuf.at[t % 2], usem.at[t % 2])

    def load_d(k):
        slot = lax.rem(k, SLOTS)
        return pltpu.make_async_copy(d.at[pl.ds(k * CI, CI)], dbuf.at[slot], dsem.at[slot])

    first = [pltpu.make_async_copy(u.at[pl.ds(e * (X // 2), X // 2), pl.ds(0, TY), :],
                                   ubuf.at[0, pl.ds(e * (X // 2), X // 2)], usem.at[2 * e]) for e in range(2)]
    for copy in first:
        copy.start()
    loads = [pltpu.make_async_copy(h, mats.at[e], msem.at[e]) for e, h in enumerate((a_hbm, b_hbm, c_hbm))]
    loads[0].start()
    load_u(1).start()
    for e in (1, 2):
        loads[e].start()

    barrier = pltpu.get_barrier_semaphore()
    for off in range(1, R):
        pl.semaphore_signal(barrier, inc=1, device_id={"row": row_peer(off)}, device_id_type=MESH)
    for off in range(1, C):
        pl.semaphore_signal(barrier, inc=1, device_id={"col": col_peer(off)}, device_id_type=MESH)

    def send_row(k, y0, ny):
        for off in range(1, R):
            p = row_peer(off)
            pltpu.make_async_remote_copy(
                src_ref=tx1.at[pl.ds(p * I + k * CI, CI), pl.ds(y0, ny), :],
                dst_ref=rx1.at[pl.ds(k * CI, CI), pl.ds(pl.multiple_of(me_r * Y + y0, TY), ny), :],
                send_sem=s1, recv_sem=r1.at[lax.rem(k, RING1)], device_id={"row": p}, device_id_type=MESH).start()

    H = I // PARTS

    def project(part, h, rhs):
        res = dot(jnp.concatenate([a[pl.ds(e * I + part * H, H), :] for e in range(R)], axis=0), rhs)
        for e in range(8):
            sb[h, pl.ds(e, R * H, stride=PITCH), :] = res[:, e * Z:(e + 1) * Z]

    def gather(part, t):
        def body(e, _):
            for i in range(H):
                row = (e * H + i) * PITCH
                parts = [sb[h, pl.ds(row, 8), :] for h in range(TY // 8)]
                tx1[e * I + part * H + i, pl.ds(t * TY, TY), :] = jnp.concatenate(parts, axis=0).astype(BF16)
            return 0

        lax.fori_loop(0, R, body, 0)

    def kept(t, h, e):
        ref = rx3 if t < Y // TY // 2 else rx1
        return ref.at[I // 2 + (t % (Y // TY // 2)) * TY + h * 8 + e]

    def second(part, t):
        def body(h, _):
            project(part, h, jnp.concatenate([kept(t, h, e)[...] for e in range(8)], axis=1))
            return 0

        lax.fori_loop(0, TY // 8, body, 0)
        gather(part, t)

    for t in range(Y // TY):
        slot = t % 2

        def spread(g, _):
            x0 = g * 32
            v = ubuf[slot, pl.ds(x0, 32)].astype(F32)
            for x in range(32):
                for h in range(TY // 8):
                    sa[h, pl.ds((x0 + x) * PITCH, 8), :] = v[x, h * 8:(h + 1) * 8, :]
            return 0

        if t == 0:
            first[0].wait()
            lax.fori_loop(0, X // 64, spread, 0)
            first[1].wait()
            lax.fori_loop(X // 64, X // 32, spread, 0)
        else:
            load_u(t).wait()
            lax.fori_loop(0, X // 32, spread, 0)
        if t + 2 < Y // TY:
            load_u(t + 2).start()
        if t == 0:
            loads[0].wait()

        def tile(h, _):
            cols = [sa[h, pl.ds(e, X, stride=PITCH), :].astype(BF16) for e in range(8)]
            for e in range(8):
                kept(t, h, e)[...] = cols[e]
            project(0, h, jnp.concatenate(cols, axis=1))
            return 0

        lax.fori_loop(0, TY // 8, tile, 0, unroll=True)
        gather(0, t)
        if t == 0:
            pl.semaphore_wait(barrier, R - 1 + C - 1)
        for k in range(EARLY):
            send_row(k, t * TY, TY)

    for k in range(EARLY, AHEAD):
        send_row(k, 0, Y)
    for k in range(DPRE):
        load_d(k).start()

    rest = [(part, t) for part in range(1, PARTS) for t in range(Y // TY)]
    for part, t in rest[:2]:
        second(part, t)
    loads[1].wait()
    loads[2].wait()
    af = a[...].astype(F32)
    keep = I - GI
    order = [af[e * I:e * I + keep] for e in range(R)] + [af[e * I + keep:(e + 1) * I] for e in range(R)]
    at_out[...] = jnp.concatenate(order, axis=0).T.astype(BF16)
    for e in (1, 2):
        mats[2 + e] = mats[e].T

    my_y = pl.ds(pl.multiple_of(me_r * Y, Y), Y)

    def to_h5(g):
        return h5.at[:, pl.ds(pl.multiple_of(me_r * keep + g * GI, GI), GI), :]

    def free2(slot):
        wait_bytes(tx2.at[slot, :, pl.ds(0, J * (C - 1)), :], s2.at[slot])

    def free3(slot):
        wait_bytes(tx3.at[slot, pl.ds(0, C - 1)], s3.at[slot])

    def free4(g, slot):
        wait_bytes(tx4.at[slot, pl.ds(0, Y * (R - 1))], s4.at[slot])

    per = GI // CI

    def step(k, _):
        @pl.when(k + AHEAD < n)
        def _():
            send_row(k + AHEAD, 0, Y)

        @pl.when(k < n)
        def _():
            slot = lax.rem(k, SLOTS)
            rx1[pl.ds(k * CI, CI), my_y, :] = tx1[pl.ds(me_r * I + k * CI, CI), :, :]
            wait_bytes(rx1.at[pl.ds(0, CI), pl.ds(0, Y * (R - 1)), :], r1.at[lax.rem(k, RING1)])

            @pl.when(k >= SLOTS)
            def _():
                free2(slot)

            res = dot(b[...], jnp.concatenate([rx1[k * CI + i] for i in range(CI)], axis=1)).astype(BF16)
            for i in range(CI):
                tx2[slot, i] = res[:, i * Z:(i + 1) * Z]
            for off in (2, 1, 3):
                p = col_peer(off)
                pltpu.make_async_remote_copy(
                    src_ref=tx2.at[slot, :, pl.ds(pl.multiple_of(p * J, J), J), :], dst_ref=rx2.at[k, me_c],
                    send_sem=s2.at[slot], recv_sem=r2.at[lax.rem(k, RING)], device_id={"col": p}, device_id_type=MESH).start()
            rx2[k, me_c] = tx2[slot, :, pl.ds(pl.multiple_of(me_c * J, J), J), :]

        def middle(m, _):
            slot = lax.rem(m, SLOTS)

            @pl.when(m + DPRE < n)
            def _():
                load_d(m + DPRE).start()

            load_d(m).wait()
            wait_bytes(rx2.at[m, pl.ds(0, C - 1)], r2.at[lax.rem(m, RING)])

            @pl.when(m >= SLOTS)
            def _():
                free3(slot)

            lhs = jnp.concatenate([rx2[m, e].reshape(CI * J, Z) for e in range(C)], axis=1)
            h3 = (dot(lhs, ct[...]) * dbuf[slot].reshape(CI * J, N)).astype(BF16)
            h4 = dot(h3, c[...]).astype(BF16)
            for e in range(C):
                tx3[slot, e] = h4[:, e * Z:(e + 1) * Z].reshape(CI, J, Z)
            for i in range(CI):
                for off in (2, 1, 3):
                    p = col_peer(off)
                    pltpu.make_async_remote_copy(
                        src_ref=tx3.at[slot, p, i], dst_ref=rx3.at[m * CI + i, pl.ds(pl.multiple_of(me_c * J, J), J), :],
                        send_sem=s3.at[slot], recv_sem=r3.at[lax.rem(m, RING) * CI + i], device_id={"col": p}, device_id_type=MESH).start()
            rx3[pl.ds(m * CI, CI), pl.ds(pl.multiple_of(me_c * J, J), J), :] = tx3[slot, me_c]
            return 0

        turn = n // 2
        lo = jnp.maximum(jnp.where(k <= turn, k - LAG0, k - LAG1), 0)
        hi = jnp.minimum(jnp.where(k < turn, k - LAG0, k - LAG1) + 1, n)
        lax.fori_loop(lo, hi, middle, 0)

        def late(o, _):
            g, q = lax.div(o, per), lax.rem(o, per)
            slot = lax.rem(g, 2)

            def arrived(i):
                wait_bytes(rx3.at[0, pl.ds(0, J * (C - 1)), :], r3.at[lax.rem(o, RING) * CI + i])

            @pl.when(o < n - per)
            def _():
                for i in range(CI):
                    arrived(i)
                res = dot(bt[...], jnp.concatenate([rx3[o * CI + i] for i in range(CI)], axis=1))
                for i in range(CI):
                    sa[0, pl.ds(q * CI + i, N, stride=GI), :] = res[:, i * Z:(i + 1) * Z]

            @pl.when(jnp.logical_and(o < n - per, q == per - 1))
            def _():
                @pl.when(g >= 2)
                def _():
                    free4(g - 2, slot)

                def pack(e, _):
                    y0 = e * 32
                    tx4[slot, pl.ds(y0, 32)] = (
                        sa[0, pl.ds(pl.multiple_of(y0 * GI, 32 * GI), 32 * GI), :].reshape(32, GI, Z).astype(BF16))
                    return 0

                lax.fori_loop(0, N // 32, pack, 0)
                for off in (4, 5, 3, 2, 6, 7, 1):
                    p = row_peer(off)
                    pltpu.make_async_remote_copy(
                        src_ref=tx4.at[slot, pl.ds(pl.multiple_of(p * Y, Y), Y)], dst_ref=to_h5(g),
                        send_sem=s4.at[slot], recv_sem=r4, device_id={"row": p}, device_id_type=MESH).start()
                to_h5(g)[...] = tx4[slot, my_y]

            @pl.when(o >= n - per)
            def _():
                for i in range(CI):
                    arrived(i)
                    tx4b[q, i] = dot(bt[...], rx3[o * CI + i]).astype(BF16)
                    row = me_r * GI + q * CI + i
                    for off in (4, 5, 3, 2, 6, 7, 1):
                        p = row_peer(off)
                        pltpu.make_async_remote_copy(
                            src_ref=tx4b.at[q, i, pl.ds(pl.multiple_of(p * Y, Y), Y), :], dst_ref=h5b.at[row],
                            send_sem=s5, recv_sem=r5, device_id={"row": p}, device_id_type=MESH).start()
                    h5b[row] = tx4b[q, i, my_y, :]
            return 0

        lo5 = jnp.maximum(jnp.where(k <= turn, k - LAG0, k - LAG1) - LAG5, 0)
        hi5 = jnp.minimum(jnp.where(k < turn, k - LAG0, k - LAG1) - LAG5 + 1, n)
        lax.fori_loop(lo5, hi5, late, 0)

        for e in range(2, len(rest)):
            pl.when(k == (e - 2) // 2)(functools.partial(second, *rest[e]))

        return 0

    lax.fori_loop(0, n + LAG1 + LAG5, step, 0)

    wait_bytes(tx1.at[pl.ds(0, I * (R - 1))], s1)
    for m in range(n - SLOTS, n):
        free2(m % SLOTS)
        free3(m % SLOTS)
    groups = I // GI - 1
    for g in (groups - 2, groups - 1):
        free4(g, g % 2)
    wait_bytes(tx4b.at[:, :, pl.ds(0, Y * (R - 1)), :], s5)
    wait_bytes(h5.at[:, pl.ds(0, keep * (R - 1)), :], r4)
    wait_bytes(h5b.at[pl.ds(0, GI * (R - 1))], r5)


def exchange(R, C, u, a, b, c, d):
    X, Y, Z = u.shape
    I, J, N = d.shape
    n = I // CI
    hb = pl.BlockSpec(memory_space=pl.ANY)
    vm = pl.BlockSpec(memory_space=pltpu.VMEM)
    DMA = pltpu.SemaphoreType.DMA
    return pl.pallas_call(
        functools.partial(exchange_kernel, R, C),
        name="exchange",
        out_shape=(pltpu.VMEM((Y, N - R * GI, Z), BF16), pltpu.VMEM((R * GI, Y, Z), BF16), pltpu.VMEM((X, N), BF16)),
        in_specs=[hb] * 5,
        out_specs=(vm, vm, vm),
        scratch_shapes=[
            pltpu.VMEM((5, N, X), BF16),
            pltpu.VMEM((2, X, TY, Z), BF16),
            pltpu.VMEM((TY // 8, X * PITCH, Z), F32),
            pltpu.VMEM((TY // 8, N // PARTS * PITCH, Z), F32),
            pltpu.VMEM((N, Y, Z), BF16),
            pltpu.VMEM((I, N, Z), BF16),
            pltpu.VMEM((SLOTS, CI, N, Z), BF16),
            pltpu.VMEM((n, C, CI, J, Z), BF16),
            pltpu.VMEM((SLOTS, C, CI, J, Z), BF16),
            pltpu.VMEM((I, N, Z), BF16),
            pltpu.VMEM((2, N, GI, Z), BF16),
            pltpu.VMEM((GI // CI, CI, N, Z), BF16),
            pltpu.VMEM((SLOTS, CI, J, N), F32),
            DMA((3,)), DMA((3,)), DMA((SLOTS,)), DMA, DMA((RING1,)), DMA((SLOTS,)), DMA((RING,)), DMA((SLOTS,)),
            DMA((RING * CI,)),
            DMA((2,)), DMA, DMA, DMA,
        ],
        compiler_params=pltpu.CompilerParams(
            collective_id=0, has_side_effects=True, vmem_limit_bytes=67043328 - 9 * 2**20),
    )(u, a, b, c, d)


def last_kernel(at, h, hb, w, buf, sc, sem):
    Y, K, Z = h.shape
    Kb, X = hb.shape[0], w.shape[0]
    XB = X // XPARTS
    T = buf.shape[2]
    copies = []
    for t in range(Y // T):
        slot = t % BUFS
        if t >= BUFS:
            for copy in copies[t - BUFS]:
                copy.wait()
        sc[...] = hb[:, t * T:(t + 1) * T, :].astype(F32).reshape(Kb * T, Z)
        rhs = jnp.concatenate(
            [jnp.concatenate([h[t * T + e], sc[pl.ds(e, Kb, stride=T), :].astype(BF16)], axis=0) for e in range(T)], axis=1)
        flat = buf.at[slot].reshape(X * T, Z)
        copies.append([])
        for m in range(XPARTS):
            res = dot(at[m * XB:(m + 1) * XB, :], rhs)
            for e in range(T):
                flat[pl.ds(m * XB * T + e, XB, stride=T), :] = res[:, e * Z:(e + 1) * Z]
            copy = pltpu.make_async_copy(
                buf.at[slot, pl.ds(m * XB, XB)], w.at[pl.ds(m * XB, XB), pl.ds(t * T, T), :], sem.at[slot, m])
            copy.start()
            copies[t].append(copy)
    for t in range(Y // T - BUFS, Y // T):
        for copy in copies[t]:
            copy.wait()


def last(at, h, hb):
    Y, K, Z = h.shape
    Kb, X = hb.shape[0], at.shape[0]
    T = 8
    vm = pl.BlockSpec(memory_space=pltpu.VMEM)
    inputs = [pltpu.with_memory_space_constraint(v, pltpu.VMEM) for v in (at, h, hb)]
    return pl.pallas_call(
        last_kernel,
        name="last",
        out_shape=jax.ShapeDtypeStruct((X, Y, Z), F32),
        in_specs=[vm, vm, vm],
        out_specs=pl.BlockSpec(memory_space=pl.ANY),
        scratch_shapes=[pltpu.VMEM((BUFS, X, T, Z), F32), pltpu.VMEM((Kb * T, Z), F32),
                        pltpu.SemaphoreType.DMA((BUFS, XPARTS))],
        compiler_params=pltpu.CompilerParams(vmem_limit_bytes=40 * 2**20),
    )(*inputs)


def solution(mesh):
    R, C = mesh.shape["row"], mesh.shape["col"]

    def local_apply(field_u, fac_a, fac_b, fac_c, diag_d):
        outs = []
        for e in range(field_u.shape[0]):
            h5, h5b, at = exchange(R, C, field_u[e], fac_a, fac_b, fac_c, diag_d)
            outs.append(last(at, h5, h5b))
        return jnp.stack(outs) if len(outs) > 1 else outs[0][None]

    spec = P("fields", None, "row", "col")
    fac = P("fields", None)
    return jax.shard_map(local_apply, mesh=mesh, in_specs=(spec, fac, fac, fac, P(("fields", "row"), "col", None)),
                         out_specs=spec, check_vma=False)
```

```python
import functools

import jax
import jax.numpy as jnp
from jax import lax
from jax.experimental import pallas as pl
from jax.experimental.pallas import tpu as pltpu
from jax.sharding import PartitionSpec as P

MESH = pl.DeviceIdType.MESH
F32, BF16 = jnp.float32, jnp.bfloat16
CI = 2
TY = 16
PITCH = 9
GI = 8
AHEAD = 4
EARLY = 1
DPRE = 3
LAG0, LAG1, LAG5 = 2, 1, 1
XPARTS = 2
BUFS = 4
SLOTS = 4
RING1, RING = 16, 8
PARTS = 4


def dot(a, b):
    return jnp.dot(a, b, preferred_element_type=F32)


def far_first(n):
    return sorted(range(1, n), key=lambda off: -min(off, n - off))


def wait_bytes(ref, sem):
    pltpu.make_async_copy(ref, ref, sem).wait()


def exchange_kernel(R, C, u, a_hbm, b_hbm, c_hbm, d, h5, h5b, at_out, mats, ubuf, sa, sb, tx1, rx1, tx2, rx2, tx3, rx3,
                    tx4, tx4b, dbuf, msem, fsem, usem, dsem, s1, r1, s2, r2, s3, r3, s4, r4, s5, r5):
    X, Y, Z = u.shape
    I, J, N = d.shape
    n = I // CI
    a, b, c, bt, ct = (mats.at[e] for e in range(5))
    me_r, me_c = lax.axis_index("row"), lax.axis_index("col")

    def row_peer(off):
        return lax.rem(me_r + off, R)

    def col_peer(off):
        return lax.rem(me_c + off, C)

    def load_u(t):
        return pltpu.make_async_copy(u.at[:, pl.ds(t * TY, TY), :], ubuf.at[t % 2], usem.at[t % 2])

    def load_d(k):
        slot = lax.rem(k, SLOTS)
        return pltpu.make_async_copy(d.at[pl.ds(k * CI, CI)], dbuf.at[slot], dsem.at[slot])

    XQ = X // 4
    first = [pltpu.make_async_copy(u.at[pl.ds(e * XQ, XQ), pl.ds(0, TY), :],
                                   ubuf.at[0, pl.ds(e * XQ, XQ)], fsem.at[e]) for e in range(4)]
    for copy in first:
        copy.start()
    loads = [pltpu.make_async_copy(h, mats.at[e], msem.at[e]) for e, h in enumerate((a_hbm, b_hbm, c_hbm))]
    loads[0].start()
    load_u(1).start()
    for e in (1, 2):
        loads[e].start()

    barrier = pltpu.get_barrier_semaphore()
    for off in range(1, R):
        pl.semaphore_signal(barrier, inc=1, device_id={"row": row_peer(off)}, device_id_type=MESH)
    for off in range(1, C):
        pl.semaphore_signal(barrier, inc=1, device_id={"col": col_peer(off)}, device_id_type=MESH)

    def send_row(k, y0, ny):
        for off in range(1, R):
            p = row_peer(off)
            pltpu.make_async_remote_copy(
                src_ref=tx1.at[pl.ds(p * I + k * CI, CI), pl.ds(y0, ny), :],
                dst_ref=rx1.at[pl.ds(k * CI, CI), pl.ds(pl.multiple_of(me_r * Y + y0, TY), ny), :],
                send_sem=s1, recv_sem=r1.at[lax.rem(k, RING1)], device_id={"row": p}, device_id_type=MESH).start()

    H = I // PARTS

    def project(part, h, rhs):
        res = dot(jnp.concatenate([a[pl.ds(e * I + part * H, H), :] for e in range(R)], axis=0), rhs)
        for e in range(8):
            sb[h, pl.ds(e, R * H, stride=PITCH), :] = res[:, e * Z:(e + 1) * Z]

    def gather(part, t):
        def body(e, _):
            for i in range(H):
                row = (e * H + i) * PITCH
                parts = [sb[h, pl.ds(row, 8), :] for h in range(TY // 8)]
                tx1[e * I + part * H + i, pl.ds(t * TY, TY), :] = jnp.concatenate(parts, axis=0).astype(BF16)
            return 0

        lax.fori_loop(0, R, body, 0)

    def kept(t, h, e):
        ref = rx3 if t < Y // TY // 2 else rx1
        return ref.at[I // 2 + (t % (Y // TY // 2)) * TY + h * 8 + e]

    def second(part, t):
        def body(h, _):
            project(part, h, jnp.concatenate([kept(t, h, e)[...] for e in range(8)], axis=1))
            return 0

        lax.fori_loop(0, TY // 8, body, 0)
        gather(part, t)

    for t in range(Y // TY):
        slot = t % 2

        def spread(g, _):
            x0 = g * 32
            v = ubuf[slot, pl.ds(x0, 32)].astype(F32)
            for x in range(32):
                for h in range(TY // 8):
                    sa[h, pl.ds((x0 + x) * PITCH, 8), :] = v[x, h * 8:(h + 1) * 8, :]
            return 0

        if t == 0:
            for e in range(4):
                first[e].wait()
                lax.fori_loop(e * XQ // 32, (e + 1) * XQ // 32, spread, 0, unroll=True)
        else:
            load_u(t).wait()
            lax.fori_loop(0, X // 32, spread, 0, unroll=4)
        if t + 2 < Y // TY:
            load_u(t + 2).start()
        if t == 0:
            loads[0].wait()

        def tile(h, _):
            cols = [sa[h, pl.ds(e, X, stride=PITCH), :].astype(BF16) for e in range(8)]
            for e in range(8):
                kept(t, h, e)[...] = cols[e]
            project(0, h, jnp.concatenate(cols, axis=1))
            return 0

        lax.fori_loop(0, TY // 8, tile, 0, unroll=True)
        gather(0, t)
        if t == 1:
            pl.semaphore_wait(barrier, R - 1 + C - 1)
        for k in range(EARLY):
            if t == 1:
                send_row(k, 0, 2 * TY)
            elif t > 1:
                send_row(k, t * TY, TY)

    for k in range(EARLY, AHEAD):
        send_row(k, 0, Y)
    for k in range(DPRE):
        load_d(k).start()

    rest = [(part, t) for part in range(1, PARTS) for t in range(Y // TY)]
    for part, t in rest[:2]:
        second(part, t)
    loads[1].wait()
    loads[2].wait()
    af = a[...].astype(F32)
    keep = I - GI
    order = [af[e * I:e * I + keep] for e in range(R)] + [af[e * I + keep:(e + 1) * I] for e in range(R)]
    at_out[...] = jnp.concatenate(order, axis=0).T.astype(BF16)
    for e in (1, 2):
        mats[2 + e] = mats[e].T

    my_y = pl.ds(pl.multiple_of(me_r * Y, Y), Y)

    def to_h5(g):
        return h5.at[:, pl.ds(pl.multiple_of(me_r * keep + g * GI, GI), GI), :]

    def free2(slot):
        wait_bytes(tx2.at[slot, :, pl.ds(0, J * (C - 1)), :], s2.at[slot])

    def free3(slot):
        wait_bytes(tx3.at[slot, pl.ds(0, C - 1)], s3.at[slot])

    def free4(g, slot):
        wait_bytes(tx4.at[slot, pl.ds(0, Y * (R - 1))], s4.at[slot])

    per = GI // CI

    def step(k, _):
        @pl.when(k + AHEAD < n)
        def _():
            send_row(k + AHEAD, 0, Y)

        @pl.when(k < n)
        def _():
            slot = lax.rem(k, SLOTS)
            rx1[pl.ds(k * CI, CI), my_y, :] = tx1[pl.ds(me_r * I + k * CI, CI), :, :]
            wait_bytes(rx1.at[pl.ds(0, CI), pl.ds(0, Y * (R - 1)), :], r1.at[lax.rem(k, RING1)])

            @pl.when(k >= SLOTS)
            def _():
                free2(slot)

            res = dot(b[...], jnp.concatenate([rx1[k * CI + i] for i in range(CI)], axis=1)).astype(BF16)
            for i in range(CI):
                tx2[slot, i] = res[:, i * Z:(i + 1) * Z]
            for off in far_first(C):
                p = col_peer(off)
                pltpu.make_async_remote_copy(
                    src_ref=tx2.at[slot, :, pl.ds(pl.multiple_of(p * J, J), J), :], dst_ref=rx2.at[k, me_c],
                    send_sem=s2.at[slot], recv_sem=r2.at[lax.rem(k, RING)], device_id={"col": p}, device_id_type=MESH).start()
            rx2[k, me_c] = tx2[slot, :, pl.ds(pl.multiple_of(me_c * J, J), J), :]

        def middle(m, _):
            slot = lax.rem(m, SLOTS)

            @pl.when(m + DPRE < n)
            def _():
                load_d(m + DPRE).start()

            load_d(m).wait()
            wait_bytes(rx2.at[m, pl.ds(0, C - 1)], r2.at[lax.rem(m, RING)])

            @pl.when(m >= SLOTS)
            def _():
                free3(slot)

            lhs = jnp.concatenate([rx2[m, e].reshape(CI * J, Z) for e in range(C)], axis=1)
            h3 = (dot(lhs, ct[...]) * dbuf[slot].reshape(CI * J, N)).astype(BF16)
            h4 = dot(h3, c[...]).astype(BF16)
            for e in range(C):
                tx3[slot, e] = h4[:, e * Z:(e + 1) * Z].reshape(CI, J, Z)
            for i in range(CI):
                for off in far_first(C):
                    p = col_peer(off)
                    pltpu.make_async_remote_copy(
                        src_ref=tx3.at[slot, p, i], dst_ref=rx3.at[m * CI + i, pl.ds(pl.multiple_of(me_c * J, J), J), :],
                        send_sem=s3.at[slot], recv_sem=r3.at[lax.rem(m, RING) * CI + i], device_id={"col": p}, device_id_type=MESH).start()
            rx3[pl.ds(m * CI, CI), pl.ds(pl.multiple_of(me_c * J, J), J), :] = tx3[slot, me_c]
            return 0

        turn = n // 2
        lo = jnp.maximum(jnp.where(k <= turn, k - LAG0, k - LAG1), 0)
        hi = jnp.minimum(jnp.where(k < turn, k - LAG0, k - LAG1) + 1, n)
        lax.fori_loop(lo, hi, middle, 0)

        def late(o, _):
            g, q = lax.div(o, per), lax.rem(o, per)
            slot = lax.rem(g, 2)

            def arrived(i):
                wait_bytes(rx3.at[0, pl.ds(0, J * (C - 1)), :], r3.at[lax.rem(o, RING) * CI + i])

            @pl.when(o < n - per)
            def _():
                for i in range(CI):
                    arrived(i)
                res = dot(bt[...], jnp.concatenate([rx3[o * CI + i] for i in range(CI)], axis=1))
                for i in range(CI):
                    sa[0, pl.ds(q * CI + i, N, stride=GI), :] = res[:, i * Z:(i + 1) * Z]

            @pl.when(jnp.logical_and(o < n - per, q == per - 1))
            def _():
                @pl.when(g >= 2)
                def _():
                    free4(g - 2, slot)

                def pack(e, _):
                    y0 = e * 32
                    tx4[slot, pl.ds(y0, 32)] = (
                        sa[0, pl.ds(pl.multiple_of(y0 * GI, 32 * GI), 32 * GI), :].reshape(32, GI, Z).astype(BF16))
                    return 0

                lax.fori_loop(0, N // 32, pack, 0)
                for off in far_first(R):
                    p = row_peer(off)
                    pltpu.make_async_remote_copy(
                        src_ref=tx4.at[slot, pl.ds(pl.multiple_of(p * Y, Y), Y)], dst_ref=to_h5(g),
                        send_sem=s4.at[slot], recv_sem=r4, device_id={"row": p}, device_id_type=MESH).start()
                to_h5(g)[...] = tx4[slot, my_y]

            @pl.when(o >= n - per)
            def _():
                for i in range(CI):
                    arrived(i)
                    tx4b[q, i] = dot(bt[...], rx3[o * CI + i]).astype(BF16)
                    row = me_r * GI + q * CI + i
                    for off in far_first(R):
                        p = row_peer(off)
                        pltpu.make_async_remote_copy(
                            src_ref=tx4b.at[q, i, pl.ds(pl.multiple_of(p * Y, Y), Y), :], dst_ref=h5b.at[row],
                            send_sem=s5, recv_sem=r5, device_id={"row": p}, device_id_type=MESH).start()
                    h5b[row] = tx4b[q, i, my_y, :]
            return 0

        lo5 = jnp.maximum(jnp.where(k <= turn, k - LAG0, k - LAG1) - LAG5, 0)
        hi5 = jnp.minimum(jnp.where(k < turn, k - LAG0, k - LAG1) - LAG5 + 1, n)
        lax.fori_loop(lo5, hi5, late, 0)

        for e in range(2, len(rest)):
            pl.when(k == (e - 2) // 2)(functools.partial(second, *rest[e]))

        return 0

    lax.fori_loop(0, n + LAG1 + LAG5, step, 0)

    wait_bytes(tx1.at[pl.ds(0, I * (R - 1))], s1)
    for m in range(n - SLOTS, n):
        free2(m % SLOTS)
        free3(m % SLOTS)
    groups = I // GI - 1
    for g in (groups - 2, groups - 1):
        free4(g, g % 2)
    wait_bytes(tx4b.at[:, :, pl.ds(0, Y * (R - 1)), :], s5)
    wait_bytes(h5.at[:, pl.ds(0, keep * (R - 1)), :], r4)
    wait_bytes(h5b.at[pl.ds(0, GI * (R - 1))], r5)


def exchange(R, C, u, a, b, c, d):
    X, Y, Z = u.shape
    I, J, N = d.shape
    n = I // CI
    hb = pl.BlockSpec(memory_space=pl.ANY)
    vm = pl.BlockSpec(memory_space=pltpu.VMEM)
    DMA = pltpu.SemaphoreType.DMA
    return pl.pallas_call(
        functools.partial(exchange_kernel, R, C),
        name="exchange",
        out_shape=(pltpu.VMEM((Y, N - R * GI, Z), BF16), pltpu.VMEM((R * GI, Y, Z), BF16), pltpu.VMEM((X, N), BF16)),
        in_specs=[hb] * 5,
        out_specs=(vm, vm, vm),
        scratch_shapes=[
            pltpu.VMEM((5, N, X), BF16),
            pltpu.VMEM((2, X, TY, Z), BF16),
            pltpu.VMEM((TY // 8, X * PITCH, Z), F32),
            pltpu.VMEM((TY // 8, N // PARTS * PITCH, Z), F32),
            pltpu.VMEM((N, Y, Z), BF16),
            pltpu.VMEM((I, N, Z), BF16),
            pltpu.VMEM((SLOTS, CI, N, Z), BF16),
            pltpu.VMEM((n, C, CI, J, Z), BF16),
            pltpu.VMEM((SLOTS, C, CI, J, Z), BF16),
            pltpu.VMEM((I, N, Z), BF16),
            pltpu.VMEM((2, N, GI, Z), BF16),
            pltpu.VMEM((GI // CI, CI, N, Z), BF16),
            pltpu.VMEM((SLOTS, CI, J, N), F32),
            DMA((3,)), DMA((4,)), DMA((2,)), DMA((SLOTS,)), DMA, DMA((RING1,)), DMA((SLOTS,)), DMA((RING,)), DMA((SLOTS,)),
            DMA((RING * CI,)),
            DMA((2,)), DMA, DMA, DMA,
        ],
        compiler_params=pltpu.CompilerParams(
            collective_id=0, has_side_effects=True, vmem_limit_bytes=67043328 - 9 * 2**20),
    )(u, a, b, c, d)


def last_kernel(at, h, hb, w, buf, sc, sem):
    Y, K, Z = h.shape
    Kb, X = hb.shape[0], w.shape[0]
    XB = X // XPARTS
    T = buf.shape[2]
    copies = []
    for t in range(Y // T):
        slot = t % BUFS
        if t >= BUFS:
            for copy in copies[t - BUFS]:
                copy.wait()
        sc[...] = hb[:, t * T:(t + 1) * T, :].astype(F32).reshape(Kb * T, Z)
        rhs = jnp.concatenate(
            [jnp.concatenate([h[t * T + e], sc[pl.ds(e, Kb, stride=T), :].astype(BF16)], axis=0) for e in range(T)], axis=1)
        flat = buf.at[slot].reshape(X * T, Z)
        copies.append([])
        for m in range(XPARTS):
            res = dot(at[m * XB:(m + 1) * XB, :], rhs)
            for e in range(T):
                flat[pl.ds(m * XB * T + e, XB, stride=T), :] = res[:, e * Z:(e + 1) * Z]
            copy = pltpu.make_async_copy(
                buf.at[slot, pl.ds(m * XB, XB)], w.at[pl.ds(m * XB, XB), pl.ds(t * T, T), :], sem.at[slot, m])
            copy.start()
            copies[t].append(copy)
    for t in range(Y // T - BUFS, Y // T):
        for copy in copies[t]:
            copy.wait()


def last(at, h, hb):
    Y, K, Z = h.shape
    Kb, X = hb.shape[0], at.shape[0]
    T = 8
    vm = pl.BlockSpec(memory_space=pltpu.VMEM)
    inputs = [pltpu.with_memory_space_constraint(v, pltpu.VMEM) for v in (at, h, hb)]
    return pl.pallas_call(
        last_kernel,
        name="last",
        out_shape=jax.ShapeDtypeStruct((X, Y, Z), F32),
        in_specs=[vm, vm, vm],
        out_specs=pl.BlockSpec(memory_space=pl.ANY),
        scratch_shapes=[pltpu.VMEM((BUFS, X, T, Z), F32), pltpu.VMEM((Kb * T, Z), F32),
                        pltpu.SemaphoreType.DMA((BUFS, XPARTS))],
        compiler_params=pltpu.CompilerParams(vmem_limit_bytes=40 * 2**20),
    )(*inputs)


def solution(mesh):
    R, C = mesh.shape["row"], mesh.shape["col"]

    def local_apply(field_u, fac_a, fac_b, fac_c, diag_d):
        outs = []
        for e in range(field_u.shape[0]):
            h5, h5b, at = exchange(R, C, field_u[e], fac_a, fac_b, fac_c, diag_d)
            outs.append(last(at, h5, h5b))
        return jnp.stack(outs) if len(outs) > 1 else outs[0][None]

    spec = P("fields", None, "row", "col")
    fac = P("fields", None)
    return jax.shard_map(local_apply, mesh=mesh, in_specs=(spec, fac, fac, fac, P(("fields", "row"), "col", None)),
                         out_specs=spec, check_vma=False)
```

```python
import functools

import jax
import jax.numpy as jnp
from jax import lax
from jax.experimental import pallas as pl
from jax.experimental.pallas import tpu as pltpu
from jax.sharding import PartitionSpec as P

MESH = pl.DeviceIdType.MESH
F32, BF16 = jnp.float32, jnp.bfloat16
CI = 2
TY = 16
PITCH = 9
GI = 8
AHEAD = 4
EARLY = 1
DPRE = 3
LAG0, LAG1, LAG5 = 2, 1, 1
XPARTS = 2
BUFS = 4
SLOTS = 4
RING1, RING = 12, 6
PARTS = 4


def dot(a, b):
    return jnp.dot(a, b, preferred_element_type=F32)


def far_first(n):
    return sorted(range(1, n), key=lambda off: -min(off, n - off))


def wait_bytes(ref, sem):
    pltpu.make_async_copy(ref, ref, sem).wait()


def exchange_kernel(R, C, u, a_hbm, b_hbm, c_hbm, d, h5, h5b, at_out, mats, ubuf, sa, sb, tx1, rx1, tx2, rx2, tx3, rx3,
                    tx4, tx4b, dbuf, msem, fsem, usem, dsem, s1, r1, s2, r2, s3, r3, s4, r4, s5, r5):
    X, Y, Z = u.shape
    I, J, N = d.shape
    n = I // CI
    a, b, c, bt, ct = (mats.at[e] for e in range(5))
    me_r, me_c = lax.axis_index("row"), lax.axis_index("col")

    def row_peer(off):
        return lax.rem(me_r + off, R)

    def col_peer(off):
        return lax.rem(me_c + off, C)

    def load_u(t):
        return pltpu.make_async_copy(u.at[:, pl.ds(t * TY, TY), :], ubuf.at[t % 2], usem.at[t % 2])

    def load_d(k):
        slot = lax.rem(k, SLOTS)
        return pltpu.make_async_copy(d.at[pl.ds(k * CI, CI)], dbuf.at[slot], dsem.at[slot])

    XQ = X // 4
    first = [pltpu.make_async_copy(u.at[pl.ds(e * XQ, XQ), pl.ds(0, TY), :],
                                   ubuf.at[0, pl.ds(e * XQ, XQ)], fsem.at[e]) for e in range(4)]
    for copy in first:
        copy.start()
    loads = [pltpu.make_async_copy(h, mats.at[e], msem.at[e]) for e, h in enumerate((a_hbm, b_hbm, c_hbm))]
    loads[0].start()
    load_u(1).start()
    for e in (1, 2):
        loads[e].start()

    barrier = pltpu.get_barrier_semaphore()
    for off in range(1, R):
        pl.semaphore_signal(barrier, inc=1, device_id={"row": row_peer(off)}, device_id_type=MESH)
    for off in range(1, C):
        pl.semaphore_signal(barrier, inc=1, device_id={"col": col_peer(off)}, device_id_type=MESH)

    def send_row(k, y0, ny):
        for off in range(1, R):
            p = row_peer(off)
            pltpu.make_async_remote_copy(
                src_ref=tx1.at[pl.ds(p * I + k * CI, CI), pl.ds(y0, ny), :],
                dst_ref=rx1.at[pl.ds(k * CI, CI), pl.ds(pl.multiple_of(me_r * Y + y0, TY), ny), :],
                send_sem=s1, recv_sem=r1.at[lax.rem(k, RING1)], device_id={"row": p}, device_id_type=MESH).start()

    H = I // PARTS

    def project(part, h, rhs):
        res = dot(jnp.concatenate([a[pl.ds(e * I + part * H, H), :] for e in range(R)], axis=0), rhs)
        for e in range(8):
            sb[h, pl.ds(e, R * H, stride=PITCH), :] = res[:, e * Z:(e + 1) * Z]

    def gather(part, t):
        def body(e, _):
            for i in range(H):
                row = (e * H + i) * PITCH
                parts = [sb[h, pl.ds(row, 8), :] for h in range(TY // 8)]
                tx1[e * I + part * H + i, pl.ds(t * TY, TY), :] = jnp.concatenate(parts, axis=0).astype(BF16)
            return 0

        lax.fori_loop(0, R, body, 0)

    def kept(t, h, e):
        ref = rx3 if t < Y // TY // 2 else rx1
        return ref.at[I // 2 + (t % (Y // TY // 2)) * TY + h * 8 + e]

    def second(part, t):
        def body(h, _):
            project(part, h, jnp.concatenate([kept(t, h, e)[...] for e in range(8)], axis=1))
            return 0

        lax.fori_loop(0, TY // 8, body, 0)
        gather(part, t)

    for t in range(Y // TY):
        slot = t % 2

        def spread(g, _):
            x0 = g * 32
            v = ubuf[slot, pl.ds(x0, 32)].astype(F32)
            for x in range(32):
                for h in range(TY // 8):
                    sa[h, pl.ds((x0 + x) * PITCH, 8), :] = v[x, h * 8:(h + 1) * 8, :]
            return 0

        if t == 0:
            for e in range(4):
                first[e].wait()
                lax.fori_loop(e * XQ // 32, (e + 1) * XQ // 32, spread, 0, unroll=True)
        else:
            load_u(t).wait()
            lax.fori_loop(0, X // 32, spread, 0, unroll=4)
        if t + 2 < Y // TY:
            load_u(t + 2).start()
        if t == 0:
            loads[0].wait()

        def tile(h, _):
            cols = [sa[h, pl.ds(e, X, stride=PITCH), :].astype(BF16) for e in range(8)]
            for e in range(8):
                kept(t, h, e)[...] = cols[e]
            project(0, h, jnp.concatenate(cols, axis=1))
            return 0

        lax.fori_loop(0, TY // 8, tile, 0, unroll=True)
        gather(0, t)
        if t == 1:
            pl.semaphore_wait(barrier, R - 1 + C - 1)
        for k in range(EARLY):
            if t == 1:
                send_row(k, 0, 2 * TY)
            elif t > 1:
                send_row(k, t * TY, TY)

    for k in range(EARLY, AHEAD):
        send_row(k, 0, Y)
    for k in range(DPRE):
        load_d(k).start()

    rest = [(part, t) for part in range(1, PARTS) for t in range(Y // TY)]
    for part, t in rest[:2]:
        second(part, t)
    loads[1].wait()
    loads[2].wait()
    af = a[...].astype(F32)
    keep = I - GI
    order = [af[e * I:e * I + keep] for e in range(R)] + [af[e * I + keep:(e + 1) * I] for e in range(R)]
    at_out[...] = jnp.concatenate(order, axis=0).T.astype(BF16)
    for e in (1, 2):
        mats[2 + e] = mats[e].T

    my_y = pl.ds(pl.multiple_of(me_r * Y, Y), Y)

    def to_h5(g):
        return h5.at[:, pl.ds(pl.multiple_of(me_r * keep + g * GI, GI), GI), :]

    def free2(slot):
        wait_bytes(tx2.at[slot, :, pl.ds(0, J * (C - 1)), :], s2.at[slot])

    def free3(slot):
        wait_bytes(tx3.at[slot, pl.ds(0, C - 1)], s3.at[slot])

    def free4(g, slot):
        wait_bytes(tx4.at[slot, pl.ds(0, Y * (R - 1))], s4.at[slot])

    per = GI // CI

    def step(k, _):
        @pl.when(k + AHEAD < n)
        def _():
            send_row(k + AHEAD, 0, Y)

        @pl.when(k < n)
        def _():
            slot = lax.rem(k, SLOTS)
            rx1[pl.ds(k * CI, CI), my_y, :] = tx1[pl.ds(me_r * I + k * CI, CI), :, :]
            wait_bytes(rx1.at[pl.ds(0, CI), pl.ds(0, Y * (R - 1)), :], r1.at[lax.rem(k, RING1)])

            @pl.when(k >= SLOTS)
            def _():
                free2(slot)

            res = dot(b[...], jnp.concatenate([rx1[k * CI + i] for i in range(CI)], axis=1)).astype(BF16)
            for i in range(CI):
                tx2[slot, i] = res[:, i * Z:(i + 1) * Z]
            for off in far_first(C):
                p = col_peer(off)
                pltpu.make_async_remote_copy(
                    src_ref=tx2.at[slot, :, pl.ds(pl.multiple_of(p * J, J), J), :], dst_ref=rx2.at[k, me_c],
                    send_sem=s2.at[slot], recv_sem=r2.at[lax.rem(k, RING)], device_id={"col": p}, device_id_type=MESH).start()
            rx2[k, me_c] = tx2[slot, :, pl.ds(pl.multiple_of(me_c * J, J), J), :]

        def middle(m, _):
            slot = lax.rem(m, SLOTS)

            @pl.when(m + DPRE < n)
            def _():
                load_d(m + DPRE).start()

            load_d(m).wait()
            wait_bytes(rx2.at[m, pl.ds(0, C - 1)], r2.at[lax.rem(m, RING)])

            @pl.when(m >= SLOTS)
            def _():
                free3(slot)

            lhs = jnp.concatenate([rx2[m, e].reshape(CI * J, Z) for e in range(C)], axis=1)
            h3 = (dot(lhs, ct[...]) * dbuf[slot].reshape(CI * J, N)).astype(BF16)
            h4 = dot(h3, c[...]).astype(BF16)
            for e in range(C):
                tx3[slot, e] = h4[:, e * Z:(e + 1) * Z].reshape(CI, J, Z)
            for i in range(CI):
                for off in far_first(C):
                    p = col_peer(off)
                    pltpu.make_async_remote_copy(
                        src_ref=tx3.at[slot, p, i], dst_ref=rx3.at[m * CI + i, pl.ds(pl.multiple_of(me_c * J, J), J), :],
                        send_sem=s3.at[slot], recv_sem=r3.at[lax.rem(m, RING) * CI + i], device_id={"col": p}, device_id_type=MESH).start()
            rx3[pl.ds(m * CI, CI), pl.ds(pl.multiple_of(me_c * J, J), J), :] = tx3[slot, me_c]
            return 0

        turn = n // 2
        lo = jnp.maximum(jnp.where(k <= turn, k - LAG0, k - LAG1), 0)
        hi = jnp.minimum(jnp.where(k < turn, k - LAG0, k - LAG1) + 1, n)
        lax.fori_loop(lo, hi, middle, 0)

        def late(o, _):
            g, q = lax.div(o, per), lax.rem(o, per)
            slot = lax.rem(g, 2)

            def arrived(i):
                wait_bytes(rx3.at[0, pl.ds(0, J * (C - 1)), :], r3.at[lax.rem(o, RING) * CI + i])

            @pl.when(o < n - per)
            def _():
                for i in range(CI):
                    arrived(i)
                res = dot(bt[...], jnp.concatenate([rx3[o * CI + i] for i in range(CI)], axis=1))
                for i in range(CI):
                    sa[0, pl.ds(q * CI + i, N, stride=GI), :] = res[:, i * Z:(i + 1) * Z]

            @pl.when(jnp.logical_and(o < n - per, q == per - 1))
            def _():
                @pl.when(g >= 2)
                def _():
                    free4(g - 2, slot)

                def pack(e, _):
                    y0 = e * 32
                    tx4[slot, pl.ds(y0, 32)] = (
                        sa[0, pl.ds(pl.multiple_of(y0 * GI, 32 * GI), 32 * GI), :].reshape(32, GI, Z).astype(BF16))
                    return 0

                lax.fori_loop(0, N // 32, pack, 0)
                for off in far_first(R):
                    p = row_peer(off)
                    pltpu.make_async_remote_copy(
                        src_ref=tx4.at[slot, pl.ds(pl.multiple_of(p * Y, Y), Y)], dst_ref=to_h5(g),
                        send_sem=s4.at[slot], recv_sem=r4, device_id={"row": p}, device_id_type=MESH).start()
                to_h5(g)[...] = tx4[slot, my_y]

            @pl.when(o >= n - per)
            def _():
                for i in range(CI):
                    arrived(i)
                    tx4b[q, i] = dot(bt[...], rx3[o * CI + i]).astype(BF16)
                    row = me_r * GI + q * CI + i
                    for off in far_first(R):
                        p = row_peer(off)
                        pltpu.make_async_remote_copy(
                            src_ref=tx4b.at[q, i, pl.ds(pl.multiple_of(p * Y, Y), Y), :], dst_ref=h5b.at[row],
                            send_sem=s5, recv_sem=r5, device_id={"row": p}, device_id_type=MESH).start()
                    h5b[row] = tx4b[q, i, my_y, :]
            return 0

        lo5 = jnp.maximum(jnp.where(k <= turn, k - LAG0, k - LAG1) - LAG5, 0)
        hi5 = jnp.minimum(jnp.where(k < turn, k - LAG0, k - LAG1) - LAG5 + 1, n)
        lax.fori_loop(lo5, hi5, late, 0)

        for e in range(2, len(rest)):
            pl.when(k == (e - 2) // 2)(functools.partial(second, *rest[e]))

        return 0

    lax.fori_loop(0, n + LAG1 + LAG5, step, 0)

    wait_bytes(tx1.at[pl.ds(0, I * (R - 1))], s1)
    for m in range(n - SLOTS, n):
        free2(m % SLOTS)
        free3(m % SLOTS)
    groups = I // GI - 1
    for g in (groups - 2, groups - 1):
        free4(g, g % 2)
    wait_bytes(tx4b.at[:, :, pl.ds(0, Y * (R - 1)), :], s5)
    wait_bytes(h5.at[:, pl.ds(0, keep * (R - 1)), :], r4)
    wait_bytes(h5b.at[pl.ds(0, GI * (R - 1))], r5)


def exchange(R, C, u, a, b, c, d):
    X, Y, Z = u.shape
    I, J, N = d.shape
    n = I // CI
    hb = pl.BlockSpec(memory_space=pl.ANY)
    vm = pl.BlockSpec(memory_space=pltpu.VMEM)
    DMA = pltpu.SemaphoreType.DMA
    return pl.pallas_call(
        functools.partial(exchange_kernel, R, C),
        name="exchange",
        out_shape=(pltpu.VMEM((Y, N - R * GI, Z), BF16), pltpu.VMEM((R * GI, Y, Z), BF16), pltpu.VMEM((X, N), BF16)),
        in_specs=[hb] * 5,
        out_specs=(vm, vm, vm),
        scratch_shapes=[
            pltpu.VMEM((5, N, X), BF16),
            pltpu.VMEM((2, X, TY, Z), BF16),
            pltpu.VMEM((TY // 8, X * PITCH, Z), F32),
            pltpu.VMEM((TY // 8, N // PARTS * PITCH, Z), F32),
            pltpu.VMEM((N, Y, Z), BF16),
            pltpu.VMEM((I, N, Z), BF16),
            pltpu.VMEM((SLOTS, CI, N, Z), BF16),
            pltpu.VMEM((n, C, CI, J, Z), BF16),
            pltpu.VMEM((SLOTS, C, CI, J, Z), BF16),
            pltpu.VMEM((I, N, Z), BF16),
            pltpu.VMEM((2, N, GI, Z), BF16),
            pltpu.VMEM((GI // CI, CI, N, Z), BF16),
            pltpu.VMEM((SLOTS, CI, J, N), F32),
            DMA((3,)), DMA((4,)), DMA((2,)), DMA((SLOTS,)), DMA, DMA((RING1,)), DMA((SLOTS,)), DMA((RING,)), DMA((SLOTS,)),
            DMA((RING * CI,)),
            DMA((2,)), DMA, DMA, DMA,
        ],
        compiler_params=pltpu.CompilerParams(
            collective_id=0, has_side_effects=True, vmem_limit_bytes=67043328 - 9 * 2**20),
    )(u, a, b, c, d)


def last_kernel(at, h, hb, w, buf, sc, sem):
    Y, K, Z = h.shape
    Kb, X = hb.shape[0], w.shape[0]
    XB = X // XPARTS
    T = buf.shape[2]
    copies = []
    for t in range(Y // T):
        slot = t % BUFS
        if t >= BUFS:
            for copy in copies[t - BUFS]:
                copy.wait()
        sc[...] = hb[:, t * T:(t + 1) * T, :].astype(F32).reshape(Kb * T, Z)
        rhs = jnp.concatenate(
            [jnp.concatenate([h[t * T + e], sc[pl.ds(e, Kb, stride=T), :].astype(BF16)], axis=0) for e in range(T)], axis=1)
        flat = buf.at[slot].reshape(X * T, Z)
        copies.append([])
        for m in range(XPARTS):
            res = dot(at[m * XB:(m + 1) * XB, :], rhs)
            for e in range(T):
                flat[pl.ds(m * XB * T + e, XB, stride=T), :] = res[:, e * Z:(e + 1) * Z]
            copy = pltpu.make_async_copy(
                buf.at[slot, pl.ds(m * XB, XB)], w.at[pl.ds(m * XB, XB), pl.ds(t * T, T), :], sem.at[slot, m])
            copy.start()
            copies[t].append(copy)
    for t in range(Y // T - BUFS, Y // T):
        for copy in copies[t]:
            copy.wait()


def last(at, h, hb):
    Y, K, Z = h.shape
    Kb, X = hb.shape[0], at.shape[0]
    T = 8
    vm = pl.BlockSpec(memory_space=pltpu.VMEM)
    inputs = [pltpu.with_memory_space_constraint(v, pltpu.VMEM) for v in (at, h, hb)]
    return pl.pallas_call(
        last_kernel,
        name="last",
        out_shape=jax.ShapeDtypeStruct((X, Y, Z), F32),
        in_specs=[vm, vm, vm],
        out_specs=pl.BlockSpec(memory_space=pl.ANY),
        scratch_shapes=[pltpu.VMEM((BUFS, X, T, Z), F32), pltpu.VMEM((Kb * T, Z), F32),
                        pltpu.SemaphoreType.DMA((BUFS, XPARTS))],
        compiler_params=pltpu.CompilerParams(vmem_limit_bytes=40 * 2**20),
    )(*inputs)


def solution(mesh):
    R, C = mesh.shape["row"], mesh.shape["col"]

    def local_apply(field_u, fac_a, fac_b, fac_c, diag_d):
        outs = []
        for e in range(field_u.shape[0]):
            h5, h5b, at = exchange(R, C, field_u[e], fac_a, fac_b, fac_c, diag_d)
            outs.append(last(at, h5, h5b))
        return jnp.stack(outs) if len(outs) > 1 else outs[0][None]

    spec = P("fields", None, "row", "col")
    fac = P("fields", None)
    return jax.shard_map(local_apply, mesh=mesh, in_specs=(spec, fac, fac, fac, P(("fields", "row"), "col", None)),
                         out_specs=spec, check_vma=False)
```
